256 devices in a mesh: groups: 2 (over z), elem: 128 (over x, y, core).
Axes of the slice: x: 8, y: 8, z: 2, core: 2. Of those that a mesh axis runs over, the one named last changes fastest.
The devices are a block of a 8x8x16 slice.
Arguments:
- snapshots: float32 [2, 4096, 16384], P(None, ('groups', 'elem')), parts along dimension 1, may hold values from -6 to 6
- delays: float32 [384, 2048], replicated, may hold values from -3 to 3
- element_order: int32 [4096], P('groups'), parts along dimension 0, may hold values from 0 to 2047, each once
- beam_table: int32 [512], P('groups'), parts along dimension 0, may hold values from 0 to 383
- band_len: int32 [8], replicated, may hold values from 1 to 32, 128 in all
Outputs:
- beams: float32 [16384, 2, 512], P('elem', None, 'groups'), parts along dimension 2
- power_db: float32 [8, 512], P(None, 'groups'), parts along dimension 1
The draws below stay inside these ranges and needn't reach their ends.
There are 2 independent parts, one for each index of `groups`. The reference program is written for one: setup_inputs(seed, part) draws one part's arguments, and reference() takes and returns one part's arrays. A program takes and returns all parts, laid end to end along the dimension named above; an argument that names none is the same for every part. Nothing has to cross between parts.
Inputs may be any that keep to these rules, and one draw needn't show every extreme that they name: `element_order`: each of 0 to 2047 appears once. `band_len`: the entries sum to 128.
All inputs are finite; a program needn't handle non-finite values.
Results may differ from the reference program's by a relative error of at most 0.0003.
Values sent between devices are 32-bit elements; how exact they have to be, the bound alone decides.
A program may use at most 128 MiB of HBM per device.

```python
import math
import jax
import jax.numpy as jnp
import numpy as np
from jax import lax

E = 2048
BEAMS = 256
DIRS = 384
BANDS = 8
UNITS = 128
BAND_MOST = 32
COLS = 16384


def place_ends(drawn, key, least, high):
    longest = drawn.shape.index(max(drawn.shape))
    spots = []
    for shift in (0, 1):
        where = [jax.random.randint(jax.random.fold_in(key, axis), (), 0, length) for axis, length in enumerate(drawn.shape)]
        where[longest] = (where[longest] + shift) % drawn.shape[longest]
        spots.append(tuple(where))
    return drawn.at[spots[0]].set(least).at[spots[1]].set(high)


def levels(key, dims, pieces, least, largest):
    factor_of, own = 1.0, jax.random.fold_in(key, 6)
    for dim, shards_of in pieces:
        draws = jnp.exp(jax.random.uniform(jax.random.fold_in(own, dim), (shards_of,), jnp.float32, least / len(pieces), largest / len(pieces)))
        factor_of = factor_of * jnp.repeat(draws, dims[dim] // shards_of).reshape([-1 if axis == dim else 1 for axis in range(len(dims))])
    return factor_of


def profile(number_of, total, limit, lean):
    loads = [(1 << 20) // math.isqrt(rank ** lean) + 1 for rank in range(2, number_of + 1)]
    rest, holding = total - limit - (number_of - 1), [1] * (number_of - 1)
    while rest > 0:
        movable = [i for i in range(number_of - 1) if holding[i] < limit]
        whole, budget = sum([loads[i] for i in movable]), rest
        for i in movable:
            more = min(limit - holding[i], max(1, budget * loads[i] // whole), rest)
            holding[i] = holding[i] + more
            rest = rest - more
    return np.array([limit] + holding)


def uneven_parts(stream_key, amount, total, most, lean):
    if amount == 2:
        one = jax.random.randint(stream_key, (), max(1, total - most), min(most, total - 1) + 1)
        return jnp.stack([one, total - one])
    sizes = jnp.asarray(profile(amount, total, most, lean), jnp.int32)
    couples = (amount - 1) // 2
    giver, taker = sizes[1:1 + 2 * couples:2], sizes[2:2 + 2 * couples:2]
    slack = jnp.minimum(giver - 1, most - taker)
    passed = jax.random.randint(jax.random.fold_in(stream_key, 1), (couples,), 0, 1 << 20) % (slack + 1)
    sizes = sizes.at[1:1 + 2 * couples:2].set(giver - passed).at[2:2 + 2 * couples:2].set(taker + passed)
    return sizes[jax.random.permutation(jax.random.fold_in(stream_key, 2), amount)]


def bell_draw(stream_key, dims, scale, most, split=(), held_as=jnp.bfloat16):
    gain = levels(stream_key, dims, split, -0.22, 0.18) if split else 1.0
    entries = jax.random.normal(stream_key, dims, jnp.float32) * scale * gain
    return jnp.minimum(jnp.maximum(entries, -most), most).astype(held_as)


def setup_inputs(seed: int = 0, part: int = 0) -> dict:
    splits = jax.random.split(jax.random.key(seed), 6)
    own_keys = jax.random.split(jax.random.fold_in(splits[5], part), 6)
    return {
        "snapshots": bell_draw(own_keys[0], (2, E, COLS), 1.0, 6.0, ((1, 128),), jnp.float32),
        "delays": jnp.clip(jax.random.uniform(splits[1], (DIRS, E), jnp.float32, -3.0, 3.0), -3.0, 3.0),
        "element_order": jax.random.permutation(own_keys[2], E).astype(jnp.int32),
        "beam_table": place_ends(jax.random.randint(own_keys[3], (BEAMS,), 0, DIRS), jax.random.fold_in(own_keys[3], 1), 0, DIRS - 1).astype(jnp.int32),
        "band_len": uneven_parts(splits[4], BANDS, UNITS, BAND_MOST, 2).astype(jnp.int32),
    }


epsilon = 1e-6


def band_of(band_len, position, unit_count):
    band_ends = jnp.cumsum(band_len).astype(jnp.int32)
    band_index = jnp.sum((band_ends <= position).astype(jnp.int32)).astype(jnp.int32)
    selector = jnp.arange(band_len.shape[0], dtype=jnp.int32) == band_index
    band_size = jnp.sum(jnp.where(selector, band_len, 0)).astype(jnp.int32)
    band_start = (jnp.sum(jnp.where(selector, band_ends, 0)).astype(jnp.int32) - band_size).astype(jnp.int32)
    frequency = (band_start.astype(jnp.float32) + 0.5 * band_size.astype(jnp.float32)) / float(unit_count)
    return frequency, band_size, selector.astype(jnp.float32)


def steering(delays, element_order, beam_table, frequency):
    delay_rows = jnp.take(delays, beam_table, axis=0)
    delay_rows = jnp.take(delay_rows, element_order, axis=1)
    phases = (2.0 * math.pi * frequency) * delay_rows
    scaling = float(delays.shape[1]) ** -0.5
    cosines = jnp.cos(phases) * scaling
    sines = -jnp.sin(phases) * scaling
    upper_rows = jnp.concatenate([cosines.T, sines.T], axis=1)
    lower_rows = jnp.concatenate([-sines.T, cosines.T], axis=1)
    return jnp.concatenate([upper_rows, lower_rows], axis=0)


def reference(snapshots, delays, element_order, beam_table, band_len):
    unit_cols = snapshots.shape[2] // UNITS
    stacked_rows = 2 * snapshots.shape[1]
    beam_count = beam_table.shape[0]

    def one_unit(position):
        frequency, band_size, selector = band_of(band_len, position, UNITS)
        weights = steering(delays, element_order, beam_table, frequency)
        window = lax.dynamic_slice_in_dim(snapshots, position * unit_cols, unit_cols, 2)
        formed = lax.dot_general(window.reshape(stacked_rows, unit_cols), weights, (((0,), (0,)), ((), ())), precision=lax.Precision.HIGHEST, preferred_element_type=jnp.float32)
        squares = jnp.sum(formed * formed, axis=0)
        power_mean = (squares[:beam_count] + squares[beam_count:]) / (band_size.astype(jnp.float32) * unit_cols)
        return formed, selector[:, None] * power_mean[None, :]

    formed_all, partials = lax.map(one_unit, jnp.arange(UNITS, dtype=jnp.int32))
    beams = formed_all.reshape(snapshots.shape[2], 2, beam_count)
    mean_power = jnp.sum(partials, axis=0)
    return beams, 10.0 * jnp.log10(mean_power + epsilon)
```

```python
import functools
import math

import jax
import jax.numpy as jnp
from jax import lax
from jax.experimental import pallas as pl
from jax.experimental.pallas import tpu as pltpu
from jax.sharding import PartitionSpec as P

NX, NY, NC = 8, 8, 2
RING = NX * NC
LANES = 128

epsilon = 1e-06

STEPS = (("A", 4), ("B", 3), ("B", -3), ("A", 2), ("A", -2), ("B", 1), ("B", -1), ("A", 0))
P3, M3, P2, M2, P1, M1, P0, M0 = range(8)

COS = (
    0.9999999890590201,
    -19.739204499453688,
    64.93911745988827,
    -85.45013953077586,
    60.16763095018129,
    -25.96759924584206,
    6.528658157862129,
)
SIN = (
    6.283185302511498,
    -41.341700405316736,
    81.60513138576982,
    -76.70301535347629,
    42.02592698341473,
    -14.899846660399582,
    3.2381375010236435,
)


def horner(coefficients, variable, scale):
    value = jnp.full_like(variable, coefficients[-1] * scale)
    for c in coefficients[-2::-1]:
        value = value * variable + c * scale
    return value


def split3(value):
    first = value.astype(jnp.bfloat16)
    rest = value - first.astype(jnp.float32)
    second = rest.astype(jnp.bfloat16)
    third = (rest - second.astype(jnp.float32)).astype(jnp.bfloat16)
    return first, second, third


def dot(a, b):
    return jnp.dot(a, b, preferred_element_type=jnp.float32)


def kernel(
    elem,
    snap,
    delays,
    order,
    table,
    bands,
    beams_out,
    power_out,
    recv,
    delays_v,
    order_v,
    table_v,
    bands_s,
    freq_s,
    gathered,
    picked,
    weights,
    outs,
    ins,
    row_buf,
    sum_buf,
    send_sem,
    recv_sem,
    local_sem,
    ring_send,
    ring_recv,
    row_sem,
    sum_sem,
):
    me = lax.axis_index(elem)
    x, y, c = me // (NY * NC), (me // NC) % NY, me % NC
    odd = (x + y) % 2
    units = NX * NY * NC
    band_count = bands.shape[0]
    beam_count = table.shape[1]
    dirs, elements = delays.shape
    depth = elements // NX
    own = snap.shape[1] * snap.shape[5]

    def at(px, py, pc):
        return {elem: (px * NY + py) * NC + pc}

    def wrap(v):
        return (v + 2 * NX) % NX

    barrier = pltpu.get_barrier_semaphore()

    def greet(t, carry):
        s = (x * NC + c + t) % RING
        pl.semaphore_signal(barrier, inc=1, device_id=at(s // NC, y, s % NC), device_id_type=pl.DeviceIdType.MESH)
        s = (y * NC + c + t) % RING
        pl.semaphore_signal(barrier, inc=1, device_id=at(x, s // NC, s % NC), device_id_type=pl.DeviceIdType.MESH)
        return carry

    lax.fori_loop(1, RING, greet, 0)

    loads = [
        pltpu.make_async_copy(bands, bands_s, local_sem.at[0]),
        pltpu.make_async_copy(order, order_v, local_sem.at[1]),
        pltpu.make_async_copy(table, table_v, local_sem.at[2]),
        pltpu.make_async_copy(delays, delays_v, local_sem.at[3]),
    ]
    for load in loads:
        load.start()
    pl.semaphore_wait(barrier, 2 * (RING - 1))

    def send(step, path, px, py, pc):
        role, off = STEPS[step]
        src = (px, wrap(py + off), pc) if path == 0 else (wrap(px + off), py, pc)
        slot = (x if path == 0 else y) * NC + c
        return pltpu.make_async_remote_copy(
            src_ref=snap.at[:, :, src[0], src[1], src[2]],
            dst_ref=recv.at[step, slot],
            send_sem=send_sem,
            recv_sem=recv_sem.at[step],
            device_id=at(px, py, pc),
            device_id_type=pl.DeviceIdType.MESH,
        )

    def keep(step, path):
        role, off = STEPS[step]
        src = (x, wrap(y + off), c) if path == 0 else (wrap(x + off), y, c)
        slot = (x if path == 0 else y) * NC + c
        return pltpu.make_async_copy(
            snap.at[:, :, src[0], src[1], src[2]], recv.at[step, slot], recv_sem.at[step]
        )

    for step, (role, off) in enumerate(STEPS):
        for path in (0, 1):
            shift = odd if (role == "A") == (path == 0) else 1 - odd

            @pl.when(shift == 0)
            def _():
                keep(step, path).start()

            @pl.when(shift == 1)
            def _():
                if path == 0:
                    send(step, path, wrap(x + 1), y, c).start()
                else:
                    send(step, path, x, wrap(y + 1), c).start()

            def others(t, carry):
                j, pc = t // NC, (c + t) % NC
                if path == 0:
                    send(step, path, wrap(x + shift + 2 * j), y, pc).start()
                else:
                    send(step, path, x, wrap(y + shift + 2 * j), pc).start()
                return carry

            lax.fori_loop(1, RING // 2, others, 0)

    loads[0].wait()
    ends, total = [], jnp.int32(0)
    for b in range(band_count):
        total = total + bands_s[b]
        ends.append(total)

    def unit_of(role, off):
        first = (x * NY + wrap(y + off)) * NC + c
        second = (wrap(x + off) * NY + y) * NC + c
        even = jnp.where(odd == 0, first, second)
        return even if role == "A" else first + second - even

    for step, (role, off) in enumerate(STEPS):
        unit = unit_of(role, off)
        frequency = jnp.float32(0)
        for b in range(band_count):
            start = ends[b] - bands_s[b]
            inside = jnp.logical_and(start <= unit, unit < ends[b])
            middle = start.astype(jnp.float32) + 0.5 * bands_s[b].astype(jnp.float32)
            frequency = frequency + jnp.where(inside, middle, 0.0)
        freq_s[step] = frequency / float(units)

    loads[1].wait()
    loads[2].wait()
    lane = lax.broadcasted_iota(jnp.int32, (8, depth), 1)
    row_order = jnp.zeros((8, depth), jnp.int32)
    group = NC * own
    for px in range(NX):
        part = jnp.broadcast_to(order_v[0:1, px * depth : (px + 1) * depth], (8, depth))
        part = pltpu.roll(part, (px - y + NX) % NX * group, 1)
        row_order = jnp.where(lane // group == px, part, row_order)
    column_order = jnp.broadcast_to(order_v[0:1, pl.ds(pl.multiple_of(x * depth, depth), depth)], (8, depth))
    order_a = jnp.where(odd == 0, row_order, column_order)
    order_b = row_order + column_order - order_a
    both = jnp.concatenate([order_a, order_b], axis=1)[0:1]

    loads[3].wait()
    gathered[...] = jnp.zeros_like(gathered)
    chunk = 256

    def pick_columns(i, carry):
        base = pl.multiple_of(i * chunk, chunk)
        rows = lax.broadcasted_iota(jnp.int32, (chunk, 2 * depth), 0) + base
        hot = jnp.where(rows == both, 1.0, 0.0).astype(jnp.bfloat16)
        one, two, three = split3(delays_v[:, pl.ds(base, chunk)])
        gathered[...] += dot(one, hot) + dot(two, hot) + dot(three, hot)
        return carry

    lax.fori_loop(0, elements // chunk, pick_columns, 0)
    wide = jnp.broadcast_to(table_v[...], (LANES, beam_count)).astype(jnp.float32)
    wide = jnp.transpose(wide)
    hots = []
    for d in range(0, dirs, LANES):
        column = (lax.broadcasted_iota(jnp.int32, (beam_count, LANES), 1) + d).astype(jnp.float32)
        hots.append(jnp.where(wide == column, 1.0, 0.0).astype(jnp.bfloat16))
    hot = jnp.concatenate(hots, axis=1)
    one, two, three = split3(gathered[...])
    rows = dot(hot, one) + dot(hot, two) + dot(hot, three)
    picked[0] = rows[:, :depth]
    picked[1] = rows[:, depth:]

    scale = float(elements) ** -0.5
    block = 32

    def steer(step, role):
        def body(i, carry):
            at_rows = pl.ds(pl.multiple_of(i * block, block), block)
            turns = freq_s[step] * picked[role, at_rows, :]
            nearest = (turns + 12582912.0) - 12582912.0
            r = turns - nearest
            s = r * r
            cosine = horner(COS, s, scale)
            sine = r * horner(SIN, s, scale)
            for n, value in ((0, cosine), (2, sine)):
                high = value.astype(jnp.bfloat16)
                weights[step, n, at_rows, :] = high
                weights[step, n + 1, at_rows, :] = (value - high.astype(jnp.float32)).astype(jnp.bfloat16)
            return carry

        lax.fori_loop(0, beam_count // block, body, 0)

    for step, (role, off) in enumerate(STEPS):
        steer(step, 0 if role == "A" else 1)

    def partial(step):
        pltpu.make_async_copy(recv.at[step], recv.at[step], recv_sem.at[step]).wait()
        data = jnp.concatenate(
            [recv[step, :, 0].reshape(depth, LANES), recv[step, :, 1].reshape(depth, LANES)], axis=1
        )
        high = data.astype(jnp.bfloat16)
        low = (data - high.astype(jnp.float32)).astype(jnp.bfloat16)
        w = weights.at[step]
        cos_part = dot(w[0], high) + dot(w[1], high) + dot(w[0], low)
        sin_part = dot(w[2], high) + dot(w[3], high) + dot(w[2], low)
        real = cos_part[:, :LANES] + sin_part[:, LANES:]
        imag = cos_part[:, LANES:] - sin_part[:, :LANES]
        return real, imag

    def neighbour(role, by):
        px_a = jnp.where(odd == 0, x, wrap(x + by))
        py_a = jnp.where(odd == 0, wrap(y + by), y)
        px_b = jnp.where(odd == 0, wrap(x + by), x)
        py_b = jnp.where(odd == 0, y, wrap(y + by))
        return at(px_a, py_a, c) if role == "A" else at(px_b, py_b, c)

    def pass_on(step, half, buf):
        role, off = STEPS[step]
        by = 1 if buf in (P3, P2, P1, P0) else -1
        return pltpu.make_async_remote_copy(
            src_ref=outs.at[step, half],
            dst_ref=ins.at[buf, half],
            send_sem=ring_send,
            recv_sem=ring_recv.at[buf, half],
            device_id=neighbour(role, by),
            device_id_type=pl.DeviceIdType.MESH,
        )

    def arrived(buf, half):
        pltpu.make_async_copy(ins.at[buf, half], ins.at[buf, half], ring_recv.at[buf, half]).wait()
        return ins[buf, half]

    def compute(step):
        real, imag = partial(step)
        outs[step, 0] = real
        outs[step, 1] = imag

    sent = 0
    compute(0)
    pass_on(0, 0, P3).start()
    pass_on(0, 1, M3).start()
    compute(1)
    pass_on(1, 1, P2).start()
    compute(2)
    pass_on(2, 0, M2).start()
    compute(3)
    outs[1, 0] += arrived(P3, 0)
    pass_on(1, 0, P2).start()
    outs[2, 1] += arrived(M3, 1)
    pass_on(2, 1, M2).start()
    compute(4)
    for half in (1, 0):
        outs[3, half] += arrived(P2, half)
        pass_on(3, half, P1).start()
        outs[4, 1 - half] += arrived(M2, 1 - half)
        pass_on(4, 1 - half, M1).start()
    compute(5)
    compute(6)
    for half in (1, 0):
        outs[5, half] += arrived(P1, half)
        pass_on(5, half, P0).start()
        outs[6, 1 - half] += arrived(M1, 1 - half)
        pass_on(6, 1 - half, M0).start()
    compute(7)
    squares = jnp.zeros((beam_count, LANES), jnp.float32)
    for half in (1, 0):
        value = outs[7, half] + arrived(P0, half) + arrived(M0, half)
        beams_out[half] = value
        squares = squares + value * value

    unit = unit_of("A", 0)
    size = jnp.float32(0)
    for b in range(band_count):
        inside = jnp.logical_and(ends[b] - bands_s[b] <= unit, unit < ends[b])
        size = size + jnp.where(inside, bands_s[b].astype(jnp.float32), 0.0)
    ones = jnp.full((8, LANES), 1.0, jnp.bfloat16)
    sums = jnp.zeros((8, beam_count), jnp.float32)
    for piece in split3(squares):
        sums = sums + lax.dot_general(ones, piece, (((1,), (1,)), ((), ())), preferred_element_type=jnp.float32)
    mine = sums / jnp.full((8, beam_count), size * float(LANES), jnp.float32)
    slot = y * NC + c
    row_buf[slot] = mine[0:1]

    def row_copy(t):
        s = (slot + t) % RING
        return pltpu.make_async_remote_copy(
            src_ref=row_buf.at[slot],
            dst_ref=row_buf.at[slot],
            send_sem=send_sem,
            recv_sem=row_sem,
            device_id=at(x, s // NC, s % NC),
            device_id_type=pl.DeviceIdType.MESH,
        )

    def start_rows(t, carry):
        row_copy(t).start()
        return carry

    lax.fori_loop(1, RING, start_rows, 0)

    band = lax.broadcasted_iota(jnp.int32, (8, beam_count), 0)
    first, last = jnp.zeros_like(band), jnp.zeros_like(band)
    for b in range(band_count):
        first = jnp.where(band == b, ends[b] - bands_s[b], first)
        last = jnp.where(band == b, ends[b], last)
    pltpu.make_async_copy(
        row_buf.at[pl.ds(0, RING - 1)], row_buf.at[pl.ds(0, RING - 1)], row_sem
    ).wait()
    mean = jnp.zeros((8, beam_count), jnp.float32)
    for s in range(RING):
        u = x * RING + s
        inside = jnp.logical_and(first <= u, u < last)
        mean = mean + jnp.where(inside, jnp.broadcast_to(row_buf[s], (8, beam_count)), 0.0)
    sum_buf[x] = mean

    def sum_copy(t):
        return pltpu.make_async_remote_copy(
            src_ref=sum_buf.at[x],
            dst_ref=sum_buf.at[x],
            send_sem=send_sem,
            recv_sem=sum_sem,
            device_id=at(wrap(x + t), y, c),
            device_id_type=pl.DeviceIdType.MESH,
        )

    def start_sums(t, carry):
        sum_copy(t).start()
        return carry

    lax.fori_loop(1, NX, start_sums, 0)
    pltpu.make_async_copy(
        sum_buf.at[pl.ds(0, NX - 1)], sum_buf.at[pl.ds(0, NX - 1)], sum_sem
    ).wait()
    total = sum_buf[0]
    for s in range(1, NX):
        total = total + sum_buf[s]
    power_out[...] = 10.0 * (jnp.log(total + epsilon) * (1.0 / math.log(10.0)))

    for step in range(7):
        pltpu.make_async_copy(recv.at[step], recv.at[step], send_sem).wait()
    half_ring = recv.at[7, pl.ds(0, RING // 2)]
    pltpu.make_async_copy(half_ring, half_ring, send_sem).wait()
    rows = row_buf.at[pl.ds(0, RING - 1)]
    pltpu.make_async_copy(rows, rows, send_sem).wait()
    rows = sum_buf.at[pl.ds(0, NX - 1)]
    pltpu.make_async_copy(rows, rows, send_sem).wait()
    rows = outs.at[pl.ds(0, 7)]
    pltpu.make_async_copy(rows, rows, ring_send).wait()


def local(elem, snapshots, delays, element_order, beam_table, band_len):
    planes, own, columns = snapshots.shape
    tiles = columns // LANES
    view = snapshots.reshape(planes, own // 8, 8, tiles, LANES).transpose(0, 1, 3, 2, 4)
    view = view.reshape(planes, own // 8, NX, NY, NC, 8, LANES)
    beam_count, elements = beam_table.shape[0], delays.shape[1]
    depth = elements // NX
    unit = (RING, planes, own // 8, 8, LANES)
    formed, decibels = pl.pallas_call(
        functools.partial(kernel, elem),
        out_shape=(
            jax.ShapeDtypeStruct((2, beam_count, LANES), jnp.float32),
            jax.ShapeDtypeStruct((band_len.shape[0], beam_count), jnp.float32),
        ),
        in_specs=[pl.BlockSpec(memory_space=pltpu.HBM)] * 5,
        out_specs=(pl.BlockSpec(memory_space=pltpu.VMEM), pl.BlockSpec(memory_space=pltpu.VMEM)),
        scratch_shapes=[
            pltpu.VMEM((8, *unit), jnp.float32),
            pltpu.VMEM(delays.shape, jnp.float32),
            pltpu.VMEM((1, elements), jnp.int32),
            pltpu.VMEM((1, beam_count), jnp.int32),
            pltpu.SMEM(band_len.shape, jnp.int32),
            pltpu.SMEM((8,), jnp.float32),
            pltpu.VMEM((delays.shape[0], 2 * depth), jnp.float32),
            pltpu.VMEM((2, beam_count, depth), jnp.float32),
            pltpu.VMEM((8, 4, beam_count, depth), jnp.bfloat16),
            pltpu.VMEM((8, 2, beam_count, LANES), jnp.float32),
            pltpu.VMEM((8, 2, beam_count, LANES), jnp.float32),
            pltpu.VMEM((RING, 1, beam_count), jnp.float32),
            pltpu.VMEM((NX, band_len.shape[0], beam_count), jnp.float32),
            pltpu.SemaphoreType.DMA(()),
            pltpu.SemaphoreType.DMA((8,)),
            pltpu.SemaphoreType.DMA((4,)),
            pltpu.SemaphoreType.DMA(()),
            pltpu.SemaphoreType.DMA((8, 2)),
            pltpu.SemaphoreType.DMA(()),
            pltpu.SemaphoreType.DMA(()),
        ],
        compiler_params=pltpu.CompilerParams(
            collective_id=1, has_side_effects=True, vmem_limit_bytes=48 * 1024 * 1024
        ),
    )(view, delays, element_order.reshape(1, elements), beam_table.reshape(1, beam_count), band_len)
    return formed.transpose(2, 0, 1), decibels


def solution(mesh):
    return jax.shard_map(
        functools.partial(local, "elem"),
        mesh=mesh,
        in_specs=(P(None, ("groups", "elem"), None), P(), P("groups"), P("groups"), P()),
        out_specs=(P("elem", None, "groups"), P(None, "groups")),
        check_vma=False,
    )
```

```python
import functools
import math

import jax
import jax.numpy as jnp
from jax import lax
from jax.experimental import pallas as pl
from jax.experimental.pallas import tpu as pltpu
from jax.sharding import PartitionSpec as P

NX, NY, NC = 8, 8, 2
RING = NX * NC
LANES = 128

epsilon = 1e-06

STEPS = (("A", 4), ("B", 3), ("B", -3), ("A", 2), ("A", -2), ("B", 1), ("B", -1), ("A", 0))
P3, M3, P2, M2, P1, M1, P0, M0 = range(8)
AHEAD = 4

COS = (
    0.9999999890590201,
    -19.739204499453688,
    64.93911745988827,
    -85.45013953077586,
    60.16763095018129,
    -25.96759924584206,
    6.528658157862129,
)
SIN = (
    6.283185302511498,
    -41.341700405316736,
    81.60513138576982,
    -76.70301535347629,
    42.02592698341473,
    -14.899846660399582,
    3.2381375010236435,
)


def horner(coefficients, variable, scale):
    value = jnp.full_like(variable, coefficients[-1] * scale)
    for c in coefficients[-2::-1]:
        value = value * variable + c * scale
    return value


def split3(value):
    first = value.astype(jnp.bfloat16)
    rest = value - first.astype(jnp.float32)
    second = rest.astype(jnp.bfloat16)
    third = (rest - second.astype(jnp.float32)).astype(jnp.bfloat16)
    return first, second, third


def dot(a, b):
    return jnp.dot(a, b, preferred_element_type=jnp.float32)


def kernel(
    elem,
    snap,
    delays,
    order,
    table,
    bands,
    beams_out,
    power_out,
    recv,
    delays_v,
    order_v,
    table_v,
    bands_s,
    freq_s,
    gathered,
    picked,
    weights,
    outs,
    ins,
    row_buf,
    sum_buf,
    send_sem,
    recv_sem,
    local_sem,
    ring_send,
    ring_recv,
    row_sem,
    sum_sem,
):
    me = lax.axis_index(elem)
    x, y, c = me // (NY * NC), (me // NC) % NY, me % NC
    odd = (x + y) % 2
    units = NX * NY * NC
    band_count = bands.shape[0]
    beam_count = table.shape[1]
    dirs, elements = delays.shape
    depth = elements // NX
    own = snap.shape[1] * snap.shape[5]

    def at(px, py, pc):
        return {elem: (px * NY + py) * NC + pc}

    def wrap(v):
        return (v + 2 * NX) % NX

    barrier = pltpu.get_barrier_semaphore()

    def greet(t, carry):
        s = (x * NC + c + t) % RING
        pl.semaphore_signal(barrier, inc=1, device_id=at(s // NC, y, s % NC), device_id_type=pl.DeviceIdType.MESH)
        s = (y * NC + c + t) % RING
        pl.semaphore_signal(barrier, inc=1, device_id=at(x, s // NC, s % NC), device_id_type=pl.DeviceIdType.MESH)
        return carry

    lax.fori_loop(1, RING, greet, 0)

    loads = [
        pltpu.make_async_copy(bands, bands_s, local_sem.at[0]),
        pltpu.make_async_copy(order, order_v, local_sem.at[1]),
        pltpu.make_async_copy(table, table_v, local_sem.at[2]),
        pltpu.make_async_copy(delays, delays_v, local_sem.at[3]),
    ]
    for load in loads:
        load.start()
    pl.semaphore_wait(barrier, 2 * (RING - 1))

    def send(step, path, px, py, pc):
        role, off = STEPS[step]
        src = (px, wrap(py + off), pc) if path == 0 else (wrap(px + off), py, pc)
        slot = (x if path == 0 else y) * NC + c
        return pltpu.make_async_remote_copy(
            src_ref=snap.at[:, :, src[0], src[1], src[2]],
            dst_ref=recv.at[step, slot],
            send_sem=send_sem,
            recv_sem=recv_sem.at[step],
            device_id=at(px, py, pc),
            device_id_type=pl.DeviceIdType.MESH,
        )

    def keep(step, path):
        role, off = STEPS[step]
        src = (x, wrap(y + off), c) if path == 0 else (wrap(x + off), y, c)
        slot = (x if path == 0 else y) * NC + c
        return pltpu.make_async_copy(
            snap.at[:, :, src[0], src[1], src[2]], recv.at[step, slot], recv_sem.at[step]
        )

    def exchange(step):
        role, off = STEPS[step]
        for path in (0, 1):
            shift = odd if (role == "A") == (path == 0) else 1 - odd

            @pl.when(shift == 0)
            def _():
                keep(step, path).start()

            @pl.when(shift == 1)
            def _():
                if path == 0:
                    send(step, path, wrap(x + 1), y, c).start()
                else:
                    send(step, path, x, wrap(y + 1), c).start()

            def others(t, carry):
                j, pc = t // NC, (c + t) % NC
                if path == 0:
                    send(step, path, wrap(x + shift + 2 * j), y, pc).start()
                else:
                    send(step, path, x, wrap(y + shift + 2 * j), pc).start()
                return carry

            lax.fori_loop(1, RING // 2, others, 0)

    for step in range(AHEAD):
        exchange(step)

    loads[0].wait()
    ends, total = [], jnp.int32(0)
    for b in range(band_count):
        total = total + bands_s[b]
        ends.append(total)

    def unit_of(role, off):
        first = (x * NY + wrap(y + off)) * NC + c
        second = (wrap(x + off) * NY + y) * NC + c
        even = jnp.where(odd == 0, first, second)
        return even if role == "A" else first + second - even

    for step, (role, off) in enumerate(STEPS):
        unit = unit_of(role, off)
        frequency = jnp.float32(0)
        for b in range(band_count):
            start = ends[b] - bands_s[b]
            inside = jnp.logical_and(start <= unit, unit < ends[b])
            middle = start.astype(jnp.float32) + 0.5 * bands_s[b].astype(jnp.float32)
            frequency = frequency + jnp.where(inside, middle, 0.0)
        freq_s[step] = frequency / float(units)

    loads[1].wait()
    loads[2].wait()
    lane = lax.broadcasted_iota(jnp.int32, (8, depth), 1)
    row_order = jnp.zeros((8, depth), jnp.int32)
    group = NC * own
    for px in range(NX):
        part = jnp.broadcast_to(order_v[0:1, px * depth : (px + 1) * depth], (8, depth))
        part = pltpu.roll(part, (px - y + NX) % NX * group, 1)
        row_order = jnp.where(lane // group == px, part, row_order)
    column_order = jnp.broadcast_to(order_v[0:1, pl.ds(pl.multiple_of(x * depth, depth), depth)], (8, depth))
    order_a = jnp.where(odd == 0, row_order, column_order)
    order_b = row_order + column_order - order_a
    both = jnp.concatenate([order_a, order_b], axis=1)[0:1]

    loads[3].wait()
    gathered[...] = jnp.zeros_like(gathered)
    chunk = 256

    def pick_columns(i, carry):
        base = pl.multiple_of(i * chunk, chunk)
        rows = lax.broadcasted_iota(jnp.int32, (chunk, 2 * depth), 0) + base
        hot = jnp.where(rows == both, 1.0, 0.0).astype(jnp.bfloat16)
        one, two, three = split3(delays_v[:, pl.ds(base, chunk)])
        gathered[...] += dot(one, hot) + dot(two, hot) + dot(three, hot)
        return carry

    lax.fori_loop(0, elements // chunk, pick_columns, 0)
    wide = jnp.broadcast_to(table_v[...], (LANES, beam_count)).astype(jnp.float32)
    wide = jnp.transpose(wide)
    hots = []
    for d in range(0, dirs, LANES):
        column = (lax.broadcasted_iota(jnp.int32, (beam_count, LANES), 1) + d).astype(jnp.float32)
        hots.append(jnp.where(wide == column, 1.0, 0.0).astype(jnp.bfloat16))
    hot = jnp.concatenate(hots, axis=1)
    one, two, three = split3(gathered[...])
    rows = dot(hot, one) + dot(hot, two) + dot(hot, three)
    picked[0] = rows[:, :depth]
    picked[1] = rows[:, depth:]

    scale = float(elements) ** -0.5
    block = 32

    def steer(step, role):
        def body(i, carry):
            at_rows = pl.ds(pl.multiple_of(i * block, block), block)
            turns = freq_s[step] * picked[role, at_rows, :]
            nearest = (turns + 12582912.0) - 12582912.0
            r = turns - nearest
            s = r * r
            cosine = horner(COS, s, scale)
            sine = r * horner(SIN, s, scale)
            for n, value in ((0, cosine), (2, sine)):
                high = value.astype(jnp.bfloat16)
                weights[step, n, at_rows, :] = high
                weights[step, n + 1, at_rows, :] = (value - high.astype(jnp.float32)).astype(jnp.bfloat16)
            return carry

        lax.fori_loop(0, beam_count // block, body, 0)

    for step, (role, off) in enumerate(STEPS):
        steer(step, 0 if role == "A" else 1)

    def partial(step):
        pltpu.make_async_copy(recv.at[step], recv.at[step], recv_sem.at[step]).wait()
        data = jnp.concatenate(
            [recv[step, :, 0].reshape(depth, LANES), recv[step, :, 1].reshape(depth, LANES)], axis=1
        )
        high = data.astype(jnp.bfloat16)
        low = (data - high.astype(jnp.float32)).astype(jnp.bfloat16)
        w = weights.at[step]
        cos_part = dot(w[0], high) + dot(w[1], high) + dot(w[0], low)
        sin_part = dot(w[2], high) + dot(w[3], high) + dot(w[2], low)
        real = cos_part[:, :LANES] + sin_part[:, LANES:]
        imag = cos_part[:, LANES:] - sin_part[:, :LANES]
        return real, imag

    def neighbour(role, by):
        px_a = jnp.where(odd == 0, x, wrap(x + by))
        py_a = jnp.where(odd == 0, wrap(y + by), y)
        px_b = jnp.where(odd == 0, wrap(x + by), x)
        py_b = jnp.where(odd == 0, y, wrap(y + by))
        return at(px_a, py_a, c) if role == "A" else at(px_b, py_b, c)

    def pass_on(step, half, buf):
        role, off = STEPS[step]
        by = 1 if buf in (P3, P2, P1, P0) else -1
        return pltpu.make_async_remote_copy(
            src_ref=outs.at[step, half],
            dst_ref=ins.at[buf, half],
            send_sem=ring_send,
            recv_sem=ring_recv.at[buf, half],
            device_id=neighbour(role, by),
            device_id_type=pl.DeviceIdType.MESH,
        )

    def arrived(buf, half):
        pltpu.make_async_copy(ins.at[buf, half], ins.at[buf, half], ring_recv.at[buf, half]).wait()
        return ins[buf, half]

    def compute(step):
        real, imag = partial(step)
        outs[step, 0] = real
        outs[step, 1] = imag

    compute(0)
    pass_on(0, 0, P3).start()
    pass_on(0, 1, M3).start()
    exchange(4)
    compute(1)
    pass_on(1, 1, P2).start()
    compute(2)
    pass_on(2, 0, M2).start()
    exchange(5)
    compute(3)
    outs[1, 0] += arrived(P3, 0)
    pass_on(1, 0, P2).start()
    outs[2, 1] += arrived(M3, 1)
    pass_on(2, 1, M2).start()
    exchange(6)
    compute(4)
    exchange(7)
    for half in (1, 0):
        outs[3, half] += arrived(P2, half)
        pass_on(3, half, P1).start()
        outs[4, 1 - half] += arrived(M2, 1 - half)
        pass_on(4, 1 - half, M1).start()
    compute(5)
    compute(6)
    for half in (1, 0):
        outs[5, half] += arrived(P1, half)
        pass_on(5, half, P0).start()
        outs[6, 1 - half] += arrived(M1, 1 - half)
        pass_on(6, 1 - half, M0).start()
    compute(7)
    squares = jnp.zeros((beam_count, LANES), jnp.float32)
    for half in (1, 0):
        value = outs[7, half] + arrived(P0, half) + arrived(M0, half)
        beams_out[half] = value
        squares = squares + value * value

    unit = unit_of("A", 0)
    size = jnp.float32(0)
    for b in range(band_count):
        inside = jnp.logical_and(ends[b] - bands_s[b] <= unit, unit < ends[b])
        size = size + jnp.where(inside, bands_s[b].astype(jnp.float32), 0.0)
    ones = jnp.full((8, LANES), 1.0, jnp.bfloat16)
    sums = jnp.zeros((8, beam_count), jnp.float32)
    for piece in split3(squares):
        sums = sums + lax.dot_general(ones, piece, (((1,), (1,)), ((), ())), preferred_element_type=jnp.float32)
    mine = sums / jnp.full((8, beam_count), size * float(LANES), jnp.float32)
    slot = y * NC + c
    row_buf[slot] = mine[0:1]

    def row_copy(t):
        s = (slot + t) % RING
        return pltpu.make_async_remote_copy(
            src_ref=row_buf.at[slot],
            dst_ref=row_buf.at[slot],
            send_sem=send_sem,
            recv_sem=row_sem,
            device_id=at(x, s // NC, s % NC),
            device_id_type=pl.DeviceIdType.MESH,
        )

    def start_rows(t, carry):
        row_copy(t).start()
        return carry

    lax.fori_loop(1, RING, start_rows, 0)

    band = lax.broadcasted_iota(jnp.int32, (8, beam_count), 0)
    first, last = jnp.zeros_like(band), jnp.zeros_like(band)
    for b in range(band_count):
        first = jnp.where(band == b, ends[b] - bands_s[b], first)
        last = jnp.where(band == b, ends[b], last)
    pltpu.make_async_copy(
        row_buf.at[pl.ds(0, RING - 1)], row_buf.at[pl.ds(0, RING - 1)], row_sem
    ).wait()
    mean = jnp.zeros((8, beam_count), jnp.float32)
    for s in range(RING):
        u = x * RING + s
        inside = jnp.logical_and(first <= u, u < last)
        mean = mean + jnp.where(inside, jnp.broadcast_to(row_buf[s], (8, beam_count)), 0.0)
    sum_buf[x] = mean

    def sum_copy(t):
        return pltpu.make_async_remote_copy(
            src_ref=sum_buf.at[x],
            dst_ref=sum_buf.at[x],
            send_sem=send_sem,
            recv_sem=sum_sem,
            device_id=at(wrap(x + t), y, c),
            device_id_type=pl.DeviceIdType.MESH,
        )

    def start_sums(t, carry):
        sum_copy(t).start()
        return carry

    lax.fori_loop(1, NX, start_sums, 0)
    pltpu.make_async_copy(
        sum_buf.at[pl.ds(0, NX - 1)], sum_buf.at[pl.ds(0, NX - 1)], sum_sem
    ).wait()
    total = sum_buf[0]
    for s in range(1, NX):
        total = total + sum_buf[s]
    power_out[...] = 10.0 * (jnp.log(total + epsilon) * (1.0 / math.log(10.0)))

    for step in range(7):
        pltpu.make_async_copy(recv.at[step], recv.at[step], send_sem).wait()
    half_ring = recv.at[7, pl.ds(0, RING // 2)]
    pltpu.make_async_copy(half_ring, half_ring, send_sem).wait()
    rows = row_buf.at[pl.ds(0, RING - 1)]
    pltpu.make_async_copy(rows, rows, send_sem).wait()
    rows = sum_buf.at[pl.ds(0, NX - 1)]
    pltpu.make_async_copy(rows, rows, send_sem).wait()
    rows = outs.at[pl.ds(0, 7)]
    pltpu.make_async_copy(rows, rows, ring_send).wait()


def local(elem, snapshots, delays, element_order, beam_table, band_len):
    planes, own, columns = snapshots.shape
    tiles = columns // LANES
    view = snapshots.reshape(planes, own // 8, 8, tiles, LANES).transpose(0, 1, 3, 2, 4)
    view = view.reshape(planes, own // 8, NX, NY, NC, 8, LANES)
    beam_count, elements = beam_table.shape[0], delays.shape[1]
    depth = elements // NX
    unit = (RING, planes, own // 8, 8, LANES)
    operands = (view, delays, element_order.reshape(1, elements), beam_table.reshape(1, beam_count), band_len)
    formed, decibels = pl.pallas_call(
        functools.partial(kernel, elem),
        out_shape=(
            jax.ShapeDtypeStruct((2, beam_count, LANES), jnp.float32),
            jax.ShapeDtypeStruct((band_len.shape[0], beam_count), jnp.float32),
        ),
        in_specs=[pl.BlockSpec(memory_space=pltpu.HBM)] * 5,
        out_specs=(pl.BlockSpec(memory_space=pltpu.VMEM), pl.BlockSpec(memory_space=pltpu.VMEM)),
        scratch_shapes=[
            pltpu.VMEM((8, *unit), jnp.float32),
            pltpu.VMEM(delays.shape, jnp.float32),
            pltpu.VMEM((1, elements), jnp.int32),
            pltpu.VMEM((1, beam_count), jnp.int32),
            pltpu.SMEM(band_len.shape, jnp.int32),
            pltpu.SMEM((8,), jnp.float32),
            pltpu.VMEM((delays.shape[0], 2 * depth), jnp.float32),
            pltpu.VMEM((2, beam_count, depth), jnp.float32),
            pltpu.VMEM((8, 4, beam_count, depth), jnp.bfloat16),
            pltpu.VMEM((8, 2, beam_count, LANES), jnp.float32),
            pltpu.VMEM((8, 2, beam_count, LANES), jnp.float32),
            pltpu.VMEM((RING, 1, beam_count), jnp.float32),
            pltpu.VMEM((NX, band_len.shape[0], beam_count), jnp.float32),
            pltpu.SemaphoreType.DMA(()),
            pltpu.SemaphoreType.DMA((8,)),
            pltpu.SemaphoreType.DMA((4,)),
            pltpu.SemaphoreType.DMA(()),
            pltpu.SemaphoreType.DMA((8, 2)),
            pltpu.SemaphoreType.DMA(()),
            pltpu.SemaphoreType.DMA(()),
        ],
        compiler_params=pltpu.CompilerParams(
            collective_id=1, has_side_effects=True, vmem_limit_bytes=48 * 1024 * 1024
        ),
    )(*(pltpu.with_memory_space_constraint(a, pltpu.HBM) for a in operands))
    return formed.transpose(2, 0, 1), decibels


def solution(mesh):
    return jax.shard_map(
        functools.partial(local, "elem"),
        mesh=mesh,
        in_specs=(P(None, ("groups", "elem"), None), P(), P("groups"), P("groups"), P()),
        out_specs=(P("elem", None, "groups"), P(None, "groups")),
        check_vma=False,
    )
```

```python
import functools
import math

import jax
import jax.numpy as jnp
from jax import lax
from jax.experimental import pallas as pl
from jax.experimental.pallas import tpu as pltpu
from jax.sharding import PartitionSpec as P

NX, NY, NC = 8, 8, 2
RING = NX * NC
LANES = 128

epsilon = 1e-06

STEPS = (("A", 4), ("B", 3), ("B", -3), ("A", 2), ("A", -2), ("B", 1), ("B", -1), ("A", 0))
P3, M3, P2, M2, P1, M1, P0, M0 = range(8)
AHEAD = 4
QUARTERS = 4

COS = (
    0.9999999890590201,
    -19.739204499453688,
    64.93911745988827,
    -85.45013953077586,
    60.16763095018129,
    -25.96759924584206,
    6.528658157862129,
)
SIN = (
    6.283185302511498,
    -41.341700405316736,
    81.60513138576982,
    -76.70301535347629,
    42.02592698341473,
    -14.899846660399582,
    3.2381375010236435,
)


def horner(coefficients, variable, scale):
    value = jnp.full_like(variable, coefficients[-1] * scale)
    for c in coefficients[-2::-1]:
        value = value * variable + c * scale
    return value


def split3(value):
    first = value.astype(jnp.bfloat16)
    rest = value - first.astype(jnp.float32)
    second = rest.astype(jnp.bfloat16)
    third = (rest - second.astype(jnp.float32)).astype(jnp.bfloat16)
    return first, second, third


def dot(a, b):
    return jnp.dot(a, b, preferred_element_type=jnp.float32)


def kernel(
    elem,
    snap,
    delays,
    order,
    table,
    bands,
    beams_out,
    power_out,
    recv,
    delays_v,
    order_v,
    table_v,
    bands_s,
    freq_s,
    gathered,
    picked,
    weights,
    outs,
    ins,
    row_buf,
    sum_buf,
    send_sem,
    recv_sem,
    local_sem,
    ring_send,
    ring_recv,
    row_sem,
    sum_sem,
    ready,
    go,
):
    me = lax.axis_index(elem)
    x, y, c = me // (NY * NC), (me // NC) % NY, me % NC
    odd = (x + y + c) % 2
    units = NX * NY * NC
    band_count = bands.shape[0]
    beam_count = table.shape[1]
    dirs, elements = delays.shape
    depth = elements // NX
    own = snap.shape[1] * snap.shape[5]

    def at(px, py, pc):
        return {elem: (px * NY + py) * NC + pc}

    def wrap(v):
        return (v + 2 * NX) % NX

    lead = c == NC - 1
    barrier = pltpu.get_barrier_semaphore()

    def tell(semaphore, target):
        pl.semaphore_signal(semaphore, inc=1, device_id=target, device_id_type=pl.DeviceIdType.MESH)

    def each_lead(act):
        @pl.when(lead)
        def _():
            def one(t, carry):
                act(wrap(x + t), wrap(y + t))
                return carry

            lax.fori_loop(1, NX, one, 0)

    def greet(px, py):
        tell(barrier, at(px, y, c))
        tell(barrier, at(x, py, c))

    tell(barrier, at(x, y, NC - 1 - c))
    each_lead(greet)

    loads = [
        pltpu.make_async_copy(bands, bands_s, local_sem.at[0]),
        pltpu.make_async_copy(order, order_v, local_sem.at[1]),
        pltpu.make_async_copy(table, table_v, local_sem.at[2]),
        pltpu.make_async_copy(delays, delays_v, local_sem.at[3]),
    ]
    for load in loads:
        load.start()
    pl.semaphore_wait(barrier, jnp.where(lead, 2 * (NX - 1) + 1, 1))

    def pass_ready(px, py):
        tell(ready.at[0, x], at(px, y, c))
        tell(ready.at[1, y], at(x, py, c))

    each_lead(pass_ready)

    @pl.when(lead)
    def _():
        tell(go, at(x, y, NC - 1 - c))

    @pl.when(jnp.logical_not(lead))
    def _():
        pl.semaphore_wait(go, 1)

    def send(step, path, px, py, pc):
        role, off = STEPS[step]
        src = (px, wrap(py + off), pc) if path == 0 else (wrap(px + off), py, pc)
        slot = (x if path == 0 else y) * NC + c
        return pltpu.make_async_remote_copy(
            src_ref=snap.at[:, :, src[0], src[1], src[2]],
            dst_ref=recv.at[step, slot],
            send_sem=send_sem,
            recv_sem=recv_sem.at[step],
            device_id=at(px, py, pc),
            device_id_type=pl.DeviceIdType.MESH,
        )

    def keep(step, path):
        role, off = STEPS[step]
        src = (x, wrap(y + off), c) if path == 0 else (wrap(x + off), y, c)
        slot = (x if path == 0 else y) * NC + c
        return pltpu.make_async_copy(
            snap.at[:, :, src[0], src[1], src[2]], recv.at[step, slot], recv_sem.at[step]
        )

    def exchange(step, pc):
        role, off = STEPS[step]
        for path in (0, 1):
            shift = (x + y + pc + (role == "B") + path) % 2
            mine = jnp.logical_and(shift == 0, c == pc)

            def away(j):
                by = shift + 2 * j
                return (wrap(x + by), y) if path == 0 else (x, wrap(y + by))

            @pl.when(mine)
            def _():
                keep(step, path).start()

            @pl.when(jnp.logical_not(mine))
            def _():
                send(step, path, *away(0), pc).start()

            def others(j, carry):
                send(step, path, *away(j), pc).start()
                return carry

            lax.fori_loop(1, NX // 2, others, 0)

    for step in range(AHEAD):
        exchange(step, NC - 1)

    def others_ready(t, carry):
        for axis, chip in ((0, wrap(x + t)), (1, wrap(y + t))):
            pl.semaphore_wait(ready.at[axis, chip], 1)

            @pl.when(lead)
            def _():
                tell(ready.at[axis, chip], at(x, y, NC - 1 - c))

        return carry

    lax.fori_loop(1, NX, others_ready, 0)
    for step in range(AHEAD):
        exchange(step, 0)
    loads[0].wait()
    ends, total = [], jnp.int32(0)
    for b in range(band_count):
        total = total + bands_s[b]
        ends.append(total)

    def unit_of(role, off):
        first = (x * NY + wrap(y + off)) * NC + c
        second = (wrap(x + off) * NY + y) * NC + c
        even = jnp.where(odd == 0, first, second)
        return even if role == "A" else first + second - even

    for step, (role, off) in enumerate(STEPS):
        unit = unit_of(role, off)
        frequency = jnp.float32(0)
        for b in range(band_count):
            start = ends[b] - bands_s[b]
            inside = jnp.logical_and(start <= unit, unit < ends[b])
            middle = start.astype(jnp.float32) + 0.5 * bands_s[b].astype(jnp.float32)
            frequency = frequency + jnp.where(inside, middle, 0.0)
        freq_s[step] = frequency / float(units)

    loads[1].wait()
    loads[2].wait()
    lane = lax.broadcasted_iota(jnp.int32, (8, depth), 1)
    row_order = jnp.zeros((8, depth), jnp.int32)
    group = NC * own
    for px in range(NX):
        part = jnp.broadcast_to(order_v[0:1, px * depth : (px + 1) * depth], (8, depth))
        part = pltpu.roll(part, (px - y + NX) % NX * group, 1)
        row_order = jnp.where(lane // group == px, part, row_order)
    column_order = jnp.broadcast_to(order_v[0:1, pl.ds(pl.multiple_of(x * depth, depth), depth)], (8, depth))
    order_a = jnp.where(odd == 0, row_order, column_order)
    order_b = row_order + column_order - order_a
    both = jnp.concatenate([order_a, order_b], axis=1)[0:1]

    loads[3].wait()
    gathered[...] = jnp.zeros_like(gathered)
    chunk = 256

    def pick_columns(i, carry):
        base = pl.multiple_of(i * chunk, chunk)
        rows = lax.broadcasted_iota(jnp.int32, (chunk, 2 * depth), 0) + base
        hot = jnp.where(rows == both, 1.0, 0.0).astype(jnp.bfloat16)
        one, two, three = split3(delays_v[:, pl.ds(base, chunk)])
        gathered[...] += dot(one, hot) + dot(two, hot) + dot(three, hot)
        return carry

    lax.fori_loop(0, elements // chunk, pick_columns, 0)
    wide = jnp.broadcast_to(table_v[...], (LANES, beam_count)).astype(jnp.float32)
    wide = jnp.transpose(wide)
    hots = []
    for d in range(0, dirs, LANES):
        column = (lax.broadcasted_iota(jnp.int32, (beam_count, LANES), 1) + d).astype(jnp.float32)
        hots.append(jnp.where(wide == column, 1.0, 0.0).astype(jnp.bfloat16))
    hot = jnp.concatenate(hots, axis=1)
    one, two, three = split3(gathered[...])
    rows = dot(hot, one) + dot(hot, two) + dot(hot, three)
    picked[0] = rows[:, :depth]
    picked[1] = rows[:, depth:]

    scale = float(elements) ** -0.5
    block = 32

    def steer(step, role):
        def body(i, carry):
            at_rows = pl.ds(pl.multiple_of(i * block, block), block)
            turns = freq_s[step] * picked[role, at_rows, :]
            nearest = (turns + 12582912.0) - 12582912.0
            r = turns - nearest
            s = r * r
            cosine = horner(COS, s, scale)
            sine = r * horner(SIN, s, scale)
            for n, value in ((0, cosine), (2, sine)):
                high = value.astype(jnp.bfloat16)
                weights[step, n, at_rows, :] = high
                weights[step, n + 1, at_rows, :] = (value - high.astype(jnp.float32)).astype(jnp.bfloat16)
            return carry

        lax.fori_loop(0, beam_count // block, body, 0)

    for step, (role, off) in enumerate(STEPS):
        steer(step, 0 if role == "A" else 1)

    def partial(step):
        pltpu.make_async_copy(recv.at[step], recv.at[step], recv_sem.at[step]).wait()
        data = jnp.concatenate(
            [recv[step, :, 0].reshape(depth, LANES), recv[step, :, 1].reshape(depth, LANES)], axis=1
        )
        high = data.astype(jnp.bfloat16)
        low = (data - high.astype(jnp.float32)).astype(jnp.bfloat16)
        w = weights.at[step]
        cos_part = dot(w[0], high) + dot(w[1], high) + dot(w[0], low)
        sin_part = dot(w[2], high) + dot(w[3], high) + dot(w[2], low)
        real = cos_part[:, :LANES] + sin_part[:, LANES:]
        imag = cos_part[:, LANES:] - sin_part[:, :LANES]
        return real, imag

    def neighbour(role, by):
        px_a = jnp.where(odd == 0, x, wrap(x + by))
        py_a = jnp.where(odd == 0, wrap(y + by), y)
        px_b = jnp.where(odd == 0, wrap(x + by), x)
        py_b = jnp.where(odd == 0, y, wrap(y + by))
        return at(px_a, py_a, c) if role == "A" else at(px_b, py_b, c)

    def pass_on(step, q, buf):
        role, off = STEPS[step]
        by = 1 if buf in (P3, P2, P1, P0) else -1
        return pltpu.make_async_remote_copy(
            src_ref=outs.at[step, q],
            dst_ref=ins.at[buf, q],
            send_sem=ring_send,
            recv_sem=ring_recv.at[buf, q],
            device_id=neighbour(role, by),
            device_id_type=pl.DeviceIdType.MESH,
        )

    def arrived(buf, q):
        pltpu.make_async_copy(ins.at[buf, q], ins.at[buf, q], ring_recv.at[buf, q]).wait()
        return ins[buf, q]

    piece = 2 * beam_count // QUARTERS

    def compute(step):
        real, imag = partial(step)
        for h, value in enumerate((real, imag)):
            for q in range(QUARTERS // 2):
                outs[step, h * (QUARTERS // 2) + q] = value[q * piece : (q + 1) * piece]

    low, high = range(QUARTERS // 2), range(QUARTERS // 2, QUARTERS)
    compute(0)
    for q in low:
        pass_on(0, q, P3).start()
    for q in high:
        pass_on(0, q, M3).start()
    for pc in range(NC):
        exchange(4, pc)
    compute(1)
    for q in high:
        pass_on(1, q, P2).start()
    compute(2)
    for q in low:
        pass_on(2, q, M2).start()
    for pc in range(NC):
        exchange(5, pc)
    compute(3)
    for p, m in zip(low, high):
        outs[1, p] += arrived(P3, p)
        pass_on(1, p, P2).start()
        outs[2, m] += arrived(M3, m)
        pass_on(2, m, M2).start()
    for pc in range(NC):
        exchange(6, pc)
    compute(4)
    for pc in range(NC):
        exchange(7, pc)
    up, down = (*high, *low), (*low, *high)
    for p, m in zip(up, down):
        outs[3, p] += arrived(P2, p)
        pass_on(3, p, P1).start()
        outs[4, m] += arrived(M2, m)
        pass_on(4, m, M1).start()
    compute(5)
    compute(6)
    for p, m in zip(up, down):
        outs[5, p] += arrived(P1, p)
        pass_on(5, p, P0).start()
        outs[6, m] += arrived(M1, m)
        pass_on(6, m, M0).start()
    compute(7)
    parts = [jnp.zeros((piece, LANES), jnp.float32) for _ in low]
    for q in up:
        value = outs[7, q] + arrived(P0, q) + arrived(M0, q)
        k = q % len(low)
        beams_out[q // len(low), k * piece : (k + 1) * piece] = value
        parts[k] = parts[k] + value * value
    squares = jnp.concatenate(parts, axis=0)

    unit = unit_of("A", 0)
    size = jnp.float32(0)
    for b in range(band_count):
        inside = jnp.logical_and(ends[b] - bands_s[b] <= unit, unit < ends[b])
        size = size + jnp.where(inside, bands_s[b].astype(jnp.float32), 0.0)
    ones = jnp.full((8, LANES), 1.0, jnp.bfloat16)
    sums = jnp.zeros((8, beam_count), jnp.float32)
    for piece in split3(squares):
        sums = sums + lax.dot_general(ones, piece, (((1,), (1,)), ((), ())), preferred_element_type=jnp.float32)
    mine = sums / jnp.full((8, beam_count), size * float(LANES), jnp.float32)
    slot = y * NC + c
    row_buf[slot] = mine[0:1]

    def row_copy(t):
        s = (slot + t) % RING
        return pltpu.make_async_remote_copy(
            src_ref=row_buf.at[slot],
            dst_ref=row_buf.at[slot],
            send_sem=send_sem,
            recv_sem=row_sem,
            device_id=at(x, s // NC, s % NC),
            device_id_type=pl.DeviceIdType.MESH,
        )

    def start_rows(t, carry):
        row_copy(t).start()
        return carry

    lax.fori_loop(1, RING, start_rows, 0)

    band = lax.broadcasted_iota(jnp.int32, (8, beam_count), 0)
    first, last = jnp.zeros_like(band), jnp.zeros_like(band)
    for b in range(band_count):
        first = jnp.where(band == b, ends[b] - bands_s[b], first)
        last = jnp.where(band == b, ends[b], last)
    pltpu.make_async_copy(
        row_buf.at[pl.ds(0, RING - 1)], row_buf.at[pl.ds(0, RING - 1)], row_sem
    ).wait()
    mean = jnp.zeros((8, beam_count), jnp.float32)
    for s in range(RING):
        u = x * RING + s
        inside = jnp.logical_and(first <= u, u < last)
        mean = mean + jnp.where(inside, jnp.broadcast_to(row_buf[s], (8, beam_count)), 0.0)
    sum_buf[x] = mean

    def sum_copy(t):
        return pltpu.make_async_remote_copy(
            src_ref=sum_buf.at[x],
            dst_ref=sum_buf.at[x],
            send_sem=send_sem,
            recv_sem=sum_sem,
            device_id=at(wrap(x + t), y, c),
            device_id_type=pl.DeviceIdType.MESH,
        )

    def start_sums(t, carry):
        sum_copy(t).start()
        return carry

    lax.fori_loop(1, NX, start_sums, 0)
    pltpu.make_async_copy(
        sum_buf.at[pl.ds(0, NX - 1)], sum_buf.at[pl.ds(0, NX - 1)], sum_sem
    ).wait()
    total = sum_buf[0]
    for s in range(1, NX):
        total = total + sum_buf[s]
    power_out[...] = 10.0 * (jnp.log(total + epsilon) * (1.0 / math.log(10.0)))

    for step in range(7):
        pltpu.make_async_copy(recv.at[step], recv.at[step], send_sem).wait()
    half_ring = recv.at[7, pl.ds(0, RING // 2)]
    pltpu.make_async_copy(half_ring, half_ring, send_sem).wait()
    rows = row_buf.at[pl.ds(0, RING - 1)]
    pltpu.make_async_copy(rows, rows, send_sem).wait()
    rows = sum_buf.at[pl.ds(0, NX - 1)]
    pltpu.make_async_copy(rows, rows, send_sem).wait()
    rows = outs.at[pl.ds(0, 7)]
    pltpu.make_async_copy(rows, rows, ring_send).wait()


def local(elem, snapshots, delays, element_order, beam_table, band_len):
    planes, own, columns = snapshots.shape
    tiles = columns // LANES
    view = snapshots.reshape(planes, own // 8, 8, tiles, LANES).transpose(0, 1, 3, 2, 4)
    view = view.reshape(planes, own // 8, NX, NY, NC, 8, LANES)
    beam_count, elements = beam_table.shape[0], delays.shape[1]
    depth = elements // NX
    unit = (RING, planes, own // 8, 8, LANES)
    operands = (view, delays, element_order.reshape(1, elements), beam_table.reshape(1, beam_count), band_len)
    formed, decibels = pl.pallas_call(
        functools.partial(kernel, elem),
        out_shape=(
            jax.ShapeDtypeStruct((2, beam_count, LANES), jnp.float32),
            jax.ShapeDtypeStruct((band_len.shape[0], beam_count), jnp.float32),
        ),
        in_specs=[pl.BlockSpec(memory_space=pltpu.HBM)] * 5,
        out_specs=(pl.BlockSpec(memory_space=pltpu.VMEM), pl.BlockSpec(memory_space=pltpu.VMEM)),
        scratch_shapes=[
            pltpu.VMEM((8, *unit), jnp.float32),
            pltpu.VMEM(delays.shape, jnp.float32),
            pltpu.VMEM((1, elements), jnp.int32),
            pltpu.VMEM((1, beam_count), jnp.int32),
            pltpu.SMEM(band_len.shape, jnp.int32),
            pltpu.SMEM((8,), jnp.float32),
            pltpu.VMEM((delays.shape[0], 2 * depth), jnp.float32),
            pltpu.VMEM((2, beam_count, depth), jnp.float32),
            pltpu.VMEM((8, 4, beam_count, depth), jnp.bfloat16),
            pltpu.VMEM((8, QUARTERS, 2 * beam_count // QUARTERS, LANES), jnp.float32),
            pltpu.VMEM((8, QUARTERS, 2 * beam_count // QUARTERS, LANES), jnp.float32),
            pltpu.VMEM((RING, 1, beam_count), jnp.float32),
            pltpu.VMEM((NX, band_len.shape[0], beam_count), jnp.float32),
            pltpu.SemaphoreType.DMA(()),
            pltpu.SemaphoreType.DMA((8,)),
            pltpu.SemaphoreType.DMA((4,)),
            pltpu.SemaphoreType.DMA(()),
            pltpu.SemaphoreType.DMA((8, QUARTERS)),
            pltpu.SemaphoreType.DMA(()),
            pltpu.SemaphoreType.DMA(()),
            pltpu.SemaphoreType.REGULAR((2, NX)),
            pltpu.SemaphoreType.REGULAR,
        ],
        compiler_params=pltpu.CompilerParams(
            collective_id=1, has_side_effects=True, vmem_limit_bytes=48 * 1024 * 1024
        ),
    )(*(pltpu.with_memory_space_constraint(a, pltpu.HBM) for a in operands))
    return formed.transpose(2, 0, 1), decibels


def solution(mesh):
    return jax.shard_map(
        functools.partial(local, "elem"),
        mesh=mesh,
        in_specs=(P(None, ("groups", "elem"), None), P(), P("groups"), P("groups"), P()),
        out_specs=(P("elem", None, "groups"), P(None, "groups")),
        check_vma=False,
    )
```

```python
import functools
import math

import jax
import jax.numpy as jnp
from jax import lax
from jax.experimental import pallas as pl
from jax.experimental.pallas import tpu as pltpu
from jax.sharding import PartitionSpec as P

NX, NY, NC = 8, 8, 2
RING = NX * NC
LANES = 128

epsilon = 1e-06

STEPS = (("A", 4), ("B", 3), ("B", -3), ("A", 2), ("A", -2), ("B", 1), ("B", -1), ("A", 0))
P3, M3, P2, M2, P1, M1, P0, M0 = range(8)
AHEAD = 7
QUARTERS = 4

COS = (
    0.9999999890590201,
    -19.739204499453688,
    64.93911745988827,
    -85.45013953077586,
    60.16763095018129,
    -25.96759924584206,
    6.528658157862129,
)
SIN = (
    6.283185302511498,
    -41.341700405316736,
    81.60513138576982,
    -76.70301535347629,
    42.02592698341473,
    -14.899846660399582,
    3.2381375010236435,
)


def horner(coefficients, variable, scale):
    value = jnp.full_like(variable, coefficients[-1] * scale)
    for c in coefficients[-2::-1]:
        value = value * variable + c * scale
    return value


def split3(value):
    first = value.astype(jnp.bfloat16)
    rest = value - first.astype(jnp.float32)
    second = rest.astype(jnp.bfloat16)
    third = (rest - second.astype(jnp.float32)).astype(jnp.bfloat16)
    return first, second, third


def dot(a, b):
    return jnp.dot(a, b, preferred_element_type=jnp.float32)


def kernel(
    elem,
    snap,
    delays,
    order,
    table,
    bands,
    beams_out,
    power_out,
    recv,
    delays_v,
    order_v,
    table_v,
    bands_s,
    freq_s,
    gathered,
    picked,
    weights,
    outs,
    ins,
    row_buf,
    sum_buf,
    send_sem,
    recv_sem,
    local_sem,
    ring_send,
    ring_recv,
    row_sem,
    sum_sem,
    ready,
    go,
):
    me = lax.axis_index(elem)
    x, y, c = me // (NY * NC), (me // NC) % NY, me % NC
    odd = (x + y + c) % 2
    units = NX * NY * NC
    band_count = bands.shape[0]
    beam_count = table.shape[1]
    dirs, elements = delays.shape
    depth = elements // NX
    own = snap.shape[1] * snap.shape[5]

    def at(px, py, pc):
        return {elem: (px * NY + py) * NC + pc}

    def wrap(v):
        return (v + 2 * NX) % NX

    lead = c == NC - 1
    barrier = pltpu.get_barrier_semaphore()

    def tell(semaphore, target):
        pl.semaphore_signal(semaphore, inc=1, device_id=target, device_id_type=pl.DeviceIdType.MESH)

    def each_lead(act):
        @pl.when(lead)
        def _():
            def one(t, carry):
                act(wrap(x + t), wrap(y + t))
                return carry

            lax.fori_loop(1, NX, one, 0)

    def greet(px, py):
        tell(barrier, at(px, y, c))
        tell(barrier, at(x, py, c))

    tell(barrier, at(x, y, NC - 1 - c))
    each_lead(greet)

    loads = [
        pltpu.make_async_copy(bands, bands_s, local_sem.at[0]),
        pltpu.make_async_copy(order, order_v, local_sem.at[1]),
        pltpu.make_async_copy(table, table_v, local_sem.at[2]),
        pltpu.make_async_copy(delays, delays_v, local_sem.at[3]),
    ]
    for load in loads:
        load.start()
    pl.semaphore_wait(barrier, jnp.where(lead, 2 * (NX - 1) + 1, 1))

    def pass_ready(px, py):
        tell(ready.at[0, x], at(px, y, c))
        tell(ready.at[1, y], at(x, py, c))

    each_lead(pass_ready)

    @pl.when(lead)
    def _():
        tell(go, at(x, y, NC - 1 - c))

    @pl.when(jnp.logical_not(lead))
    def _():
        pl.semaphore_wait(go, 1)

    def send(step, path, px, py, pc):
        role, off = STEPS[step]
        src = (px, wrap(py + off), pc) if path == 0 else (wrap(px + off), py, pc)
        slot = (x if path == 0 else y) * NC + c
        return pltpu.make_async_remote_copy(
            src_ref=snap.at[:, :, src[0], src[1], src[2]],
            dst_ref=recv.at[step, slot],
            send_sem=send_sem,
            recv_sem=recv_sem.at[step],
            device_id=at(px, py, pc),
            device_id_type=pl.DeviceIdType.MESH,
        )

    def keep(step, path):
        role, off = STEPS[step]
        src = (x, wrap(y + off), c) if path == 0 else (wrap(x + off), y, c)
        slot = (x if path == 0 else y) * NC + c
        return pltpu.make_async_copy(
            snap.at[:, :, src[0], src[1], src[2]], recv.at[step, slot], recv_sem.at[step]
        )

    def exchange(step, pc):
        role, off = STEPS[step]
        for path in (0, 1):
            shift = (x + y + pc + (role == "B") + path) % 2
            mine = jnp.logical_and(shift == 0, c == pc)

            def away(j):
                by = shift + 2 * j
                return (wrap(x + by), y) if path == 0 else (x, wrap(y + by))

            @pl.when(mine)
            def _():
                keep(step, path).start()

            @pl.when(jnp.logical_not(mine))
            def _():
                send(step, path, *away(0), pc).start()

            def others(j, carry):
                send(step, path, *away(j), pc).start()
                return carry

            lax.fori_loop(1, NX // 2, others, 0)

    for step in range(AHEAD):
        exchange(step, NC - 1)

    def others_ready(t, carry):
        for axis, chip in ((0, wrap(x + t)), (1, wrap(y + t))):
            pl.semaphore_wait(ready.at[axis, chip], 1)

            @pl.when(lead)
            def _():
                tell(ready.at[axis, chip], at(x, y, NC - 1 - c))

        return carry

    lax.fori_loop(1, NX, others_ready, 0)
    for step in range(AHEAD):
        exchange(step, 0)
    loads[0].wait()
    ends, total = [], jnp.int32(0)
    for b in range(band_count):
        total = total + bands_s[b]
        ends.append(total)

    def unit_of(role, off):
        first = (x * NY + wrap(y + off)) * NC + c
        second = (wrap(x + off) * NY + y) * NC + c
        even = jnp.where(odd == 0, first, second)
        return even if role == "A" else first + second - even

    for step, (role, off) in enumerate(STEPS):
        unit = unit_of(role, off)
        frequency = jnp.float32(0)
        for b in range(band_count):
            start = ends[b] - bands_s[b]
            inside = jnp.logical_and(start <= unit, unit < ends[b])
            middle = start.astype(jnp.float32) + 0.5 * bands_s[b].astype(jnp.float32)
            frequency = frequency + jnp.where(inside, middle, 0.0)
        freq_s[step] = frequency / float(units)

    loads[1].wait()
    loads[2].wait()
    lane = lax.broadcasted_iota(jnp.int32, (8, depth), 1)
    row_order = jnp.zeros((8, depth), jnp.int32)
    group = NC * own
    for px in range(NX):
        part = jnp.broadcast_to(order_v[0:1, px * depth : (px + 1) * depth], (8, depth))
        part = pltpu.roll(part, (px - y + NX) % NX * group, 1)
        row_order = jnp.where(lane // group == px, part, row_order)
    column_order = jnp.broadcast_to(order_v[0:1, pl.ds(pl.multiple_of(x * depth, depth), depth)], (8, depth))
    order_a = jnp.where(odd == 0, row_order, column_order)
    order_b = row_order + column_order - order_a
    both = jnp.concatenate([order_a, order_b], axis=1)[0:1]

    loads[3].wait()
    gathered[...] = jnp.zeros_like(gathered)
    chunk = 256

    def pick_columns(i, carry):
        base = pl.multiple_of(i * chunk, chunk)
        rows = lax.broadcasted_iota(jnp.int32, (chunk, 2 * depth), 0) + base
        hot = jnp.where(rows == both, 1.0, 0.0).astype(jnp.bfloat16)
        one, two, three = split3(delays_v[:, pl.ds(base, chunk)])
        gathered[...] += dot(one, hot) + dot(two, hot) + dot(three, hot)
        return carry

    lax.fori_loop(0, elements // chunk, pick_columns, 0)
    wide = jnp.broadcast_to(table_v[...], (LANES, beam_count)).astype(jnp.float32)
    wide = jnp.transpose(wide)
    hots = []
    for d in range(0, dirs, LANES):
        column = (lax.broadcasted_iota(jnp.int32, (beam_count, LANES), 1) + d).astype(jnp.float32)
        hots.append(jnp.where(wide == column, 1.0, 0.0).astype(jnp.bfloat16))
    hot = jnp.concatenate(hots, axis=1)
    one, two, three = split3(gathered[...])
    rows = dot(hot, one) + dot(hot, two) + dot(hot, three)
    picked[0] = rows[:, :depth]
    picked[1] = rows[:, depth:]

    scale = float(elements) ** -0.5
    block = 32

    def steer(step, role):
        def body(i, carry):
            at_rows = pl.ds(pl.multiple_of(i * block, block), block)
            turns = freq_s[step] * picked[role, at_rows, :]
            nearest = (turns + 12582912.0) - 12582912.0
            r = turns - nearest
            s = r * r
            cosine = horner(COS, s, scale)
            sine = r * horner(SIN, s, scale)
            for n, value in ((0, cosine), (2, sine)):
                high = value.astype(jnp.bfloat16)
                weights[step, n, at_rows, :] = high
                weights[step, n + 1, at_rows, :] = (value - high.astype(jnp.float32)).astype(jnp.bfloat16)
            return carry

        lax.fori_loop(0, beam_count // block, body, 0)

    for step, (role, off) in enumerate(STEPS):
        steer(step, 0 if role == "A" else 1)

    def partial(step):
        pltpu.make_async_copy(recv.at[step], recv.at[step], recv_sem.at[step]).wait()
        data = jnp.concatenate(
            [recv[step, :, 0].reshape(depth, LANES), recv[step, :, 1].reshape(depth, LANES)], axis=1
        )
        high = data.astype(jnp.bfloat16)
        low = (data - high.astype(jnp.float32)).astype(jnp.bfloat16)
        w = weights.at[step]
        cos_part = dot(w[0], high) + dot(w[1], high) + dot(w[0], low)
        sin_part = dot(w[2], high) + dot(w[3], high) + dot(w[2], low)
        real = cos_part[:, :LANES] + sin_part[:, LANES:]
        imag = cos_part[:, LANES:] - sin_part[:, :LANES]
        return real, imag

    def neighbour(role, by):
        px_a = jnp.where(odd == 0, x, wrap(x + by))
        py_a = jnp.where(odd == 0, wrap(y + by), y)
        px_b = jnp.where(odd == 0, wrap(x + by), x)
        py_b = jnp.where(odd == 0, y, wrap(y + by))
        return at(px_a, py_a, c) if role == "A" else at(px_b, py_b, c)

    def pass_on(step, q, buf):
        role, off = STEPS[step]
        by = 1 if buf in (P3, P2, P1, P0) else -1
        return pltpu.make_async_remote_copy(
            src_ref=outs.at[step, q],
            dst_ref=ins.at[buf, q],
            send_sem=ring_send,
            recv_sem=ring_recv.at[buf, q],
            device_id=neighbour(role, by),
            device_id_type=pl.DeviceIdType.MESH,
        )

    def arrived(buf, q):
        pltpu.make_async_copy(ins.at[buf, q], ins.at[buf, q], ring_recv.at[buf, q]).wait()
        return ins[buf, q]

    piece = 2 * beam_count // QUARTERS

    def compute(step):
        real, imag = partial(step)
        for h, value in enumerate((real, imag)):
            for q in range(QUARTERS // 2):
                outs[step, h * (QUARTERS // 2) + q] = value[q * piece : (q + 1) * piece]

    low, high = range(QUARTERS // 2), range(QUARTERS // 2, QUARTERS)
    compute(0)
    for q in low:
        pass_on(0, q, P3).start()
    for q in high:
        pass_on(0, q, M3).start()
    compute(1)
    for q in high:
        pass_on(1, q, P2).start()
    compute(2)
    for q in low:
        pass_on(2, q, M2).start()
    compute(3)
    for p, m in zip(low, high):
        outs[1, p] += arrived(P3, p)
        pass_on(1, p, P2).start()
        outs[2, m] += arrived(M3, m)
        pass_on(2, m, M2).start()
    compute(4)
    up, down = (*high, *low), (*low, *high)
    for p, m in zip(up, down):
        outs[3, p] += arrived(P2, p)
        pass_on(3, p, P1).start()
        outs[4, m] += arrived(M2, m)
        pass_on(4, m, M1).start()
    for pc in range(NC):
        exchange(7, pc)
    compute(5)
    compute(6)
    for p, m in zip(up, down):
        outs[5, p] += arrived(P1, p)
        pass_on(5, p, P0).start()
        outs[6, m] += arrived(M1, m)
        pass_on(6, m, M0).start()
    compute(7)
    parts = [jnp.zeros((piece, LANES), jnp.float32) for _ in low]
    for q in up:
        value = outs[7, q] + arrived(P0, q) + arrived(M0, q)
        k = q % len(low)
        beams_out[q // len(low), k * piece : (k + 1) * piece] = value
        parts[k] = parts[k] + value * value
    squares = jnp.concatenate(parts, axis=0)

    unit = unit_of("A", 0)
    size = jnp.float32(0)
    for b in range(band_count):
        inside = jnp.logical_and(ends[b] - bands_s[b] <= unit, unit < ends[b])
        size = size + jnp.where(inside, bands_s[b].astype(jnp.float32), 0.0)
    ones = jnp.full((8, LANES), 1.0, jnp.bfloat16)
    sums = jnp.zeros((8, beam_count), jnp.float32)
    for piece in split3(squares):
        sums = sums + lax.dot_general(ones, piece, (((1,), (1,)), ((), ())), preferred_element_type=jnp.float32)
    mine = sums / jnp.full((8, beam_count), size * float(LANES), jnp.float32)
    slot = y * NC + c
    row_buf[slot] = mine[0:1]

    def row_copy(t):
        s = (slot + t) % RING
        return pltpu.make_async_remote_copy(
            src_ref=row_buf.at[slot],
            dst_ref=row_buf.at[slot],
            send_sem=send_sem,
            recv_sem=row_sem,
            device_id=at(x, s // NC, s % NC),
            device_id_type=pl.DeviceIdType.MESH,
        )

    def start_rows(t, carry):
        row_copy(t).start()
        return carry

    lax.fori_loop(1, RING, start_rows, 0)

    band = lax.broadcasted_iota(jnp.int32, (8, beam_count), 0)
    first, last = jnp.zeros_like(band), jnp.zeros_like(band)
    for b in range(band_count):
        first = jnp.where(band == b, ends[b] - bands_s[b], first)
        last = jnp.where(band == b, ends[b], last)
    pltpu.make_async_copy(
        row_buf.at[pl.ds(0, RING - 1)], row_buf.at[pl.ds(0, RING - 1)], row_sem
    ).wait()
    mean = jnp.zeros((8, beam_count), jnp.float32)
    for s in range(RING):
        u = x * RING + s
        inside = jnp.logical_and(first <= u, u < last)
        mean = mean + jnp.where(inside, jnp.broadcast_to(row_buf[s], (8, beam_count)), 0.0)
    sum_buf[x] = mean

    def sum_copy(t):
        return pltpu.make_async_remote_copy(
            src_ref=sum_buf.at[x],
            dst_ref=sum_buf.at[x],
            send_sem=send_sem,
            recv_sem=sum_sem,
            device_id=at(wrap(x + t), y, c),
            device_id_type=pl.DeviceIdType.MESH,
        )

    def start_sums(t, carry):
        sum_copy(t).start()
        return carry

    lax.fori_loop(1, NX, start_sums, 0)
    pltpu.make_async_copy(
        sum_buf.at[pl.ds(0, NX - 1)], sum_buf.at[pl.ds(0, NX - 1)], sum_sem
    ).wait()
    total = sum_buf[0]
    for s in range(1, NX):
        total = total + sum_buf[s]
    power_out[...] = 10.0 * (jnp.log(total + epsilon) * (1.0 / math.log(10.0)))

    for step in range(7):
        pltpu.make_async_copy(recv.at[step], recv.at[step], send_sem).wait()
    half_ring = recv.at[7, pl.ds(0, RING // 2)]
    pltpu.make_async_copy(half_ring, half_ring, send_sem).wait()
    rows = row_buf.at[pl.ds(0, RING - 1)]
    pltpu.make_async_copy(rows, rows, send_sem).wait()
    rows = sum_buf.at[pl.ds(0, NX - 1)]
    pltpu.make_async_copy(rows, rows, send_sem).wait()
    rows = outs.at[pl.ds(0, 7)]
    pltpu.make_async_copy(rows, rows, ring_send).wait()


def local(elem, snapshots, delays, element_order, beam_table, band_len):
    planes, own, columns = snapshots.shape
    tiles = columns // LANES
    view = snapshots.reshape(planes, own // 8, 8, tiles, LANES).transpose(0, 1, 3, 2, 4)
    view = view.reshape(planes, own // 8, NX, NY, NC, 8, LANES)
    beam_count, elements = beam_table.shape[0], delays.shape[1]
    depth = elements // NX
    unit = (RING, planes, own // 8, 8, LANES)
    operands = (view, delays, element_order.reshape(1, elements), beam_table.reshape(1, beam_count), band_len)
    formed, decibels = pl.pallas_call(
        functools.partial(kernel, elem),
        out_shape=(
            jax.ShapeDtypeStruct((2, beam_count, LANES), jnp.float32),
            jax.ShapeDtypeStruct((band_len.shape[0], beam_count), jnp.float32),
        ),
        in_specs=[pl.BlockSpec(memory_space=pltpu.HBM)] * 5,
        out_specs=(pl.BlockSpec(memory_space=pltpu.VMEM), pl.BlockSpec(memory_space=pltpu.VMEM)),
        scratch_shapes=[
            pltpu.VMEM((8, *unit), jnp.float32),
            pltpu.VMEM(delays.shape, jnp.float32),
            pltpu.VMEM((1, elements), jnp.int32),
            pltpu.VMEM((1, beam_count), jnp.int32),
            pltpu.SMEM(band_len.shape, jnp.int32),
            pltpu.SMEM((8,), jnp.float32),
            pltpu.VMEM((delays.shape[0], 2 * depth), jnp.float32),
            pltpu.VMEM((2, beam_count, depth), jnp.float32),
            pltpu.VMEM((8, 4, beam_count, depth), jnp.bfloat16),
            pltpu.VMEM((8, QUARTERS, 2 * beam_count // QUARTERS, LANES), jnp.float32),
            pltpu.VMEM((8, QUARTERS, 2 * beam_count // QUARTERS, LANES), jnp.float32),
            pltpu.VMEM((RING, 1, beam_count), jnp.float32),
            pltpu.VMEM((NX, band_len.shape[0], beam_count), jnp.float32),
            pltpu.SemaphoreType.DMA(()),
            pltpu.SemaphoreType.DMA((8,)),
            pltpu.SemaphoreType.DMA((4,)),
            pltpu.SemaphoreType.DMA(()),
            pltpu.SemaphoreType.DMA((8, QUARTERS)),
            pltpu.SemaphoreType.DMA(()),
            pltpu.SemaphoreType.DMA(()),
            pltpu.SemaphoreType.REGULAR((2, NX)),
            pltpu.SemaphoreType.REGULAR,
        ],
        compiler_params=pltpu.CompilerParams(
            collective_id=1, has_side_effects=True, vmem_limit_bytes=48 * 1024 * 1024
        ),
    )(*(pltpu.with_memory_space_constraint(a, pltpu.HBM) for a in operands))
    return formed.transpose(2, 0, 1), decibels


def solution(mesh):
    return jax.shard_map(
        functools.partial(local, "elem"),
        mesh=mesh,
        in_specs=(P(None, ("groups", "elem"), None), P(), P("groups"), P("groups"), P()),
        out_specs=(P("elem", None, "groups"), P(None, "groups")),
        check_vma=False,
    )
```

```python
import functools
import math

import jax
import jax.numpy as jnp
from jax import lax
from jax.experimental import pallas as pl
from jax.experimental.pallas import tpu as pltpu
from jax.sharding import PartitionSpec as P

NX, NY, NC = 8, 8, 2
RING = NX * NC
LANES = 128

epsilon = 1e-06

STEPS = (("A", 4), ("B", 3), ("B", -3), ("A", 2), ("A", -2), ("B", 1), ("B", -1), ("A", 0))
P3, M3, P2, M2, P1, M1, P0, M0 = range(8)
AHEAD = 7
QUARTERS = 4

COS = (
    0.9999999890590201,
    -19.739204499453688,
    64.93911745988827,
    -85.45013953077586,
    60.16763095018129,
    -25.96759924584206,
    6.528658157862129,
)
SIN = (
    6.283185302511498,
    -41.341700405316736,
    81.60513138576982,
    -76.70301535347629,
    42.02592698341473,
    -14.899846660399582,
    3.2381375010236435,
)


def horner(coefficients, variable, scale):
    value = jnp.full_like(variable, coefficients[-1] * scale)
    for c in coefficients[-2::-1]:
        value = value * variable + c * scale
    return value


def split3(value):
    first = value.astype(jnp.bfloat16)
    rest = value - first.astype(jnp.float32)
    second = rest.astype(jnp.bfloat16)
    third = (rest - second.astype(jnp.float32)).astype(jnp.bfloat16)
    return first, second, third


def dot(a, b):
    return jnp.dot(a, b, preferred_element_type=jnp.float32)


def kernel(
    elem,
    snap,
    delays,
    order,
    table,
    bands,
    beams_out,
    power_out,
    recv,
    delays_v,
    order_v,
    table_v,
    bands_s,
    freq_s,
    gathered,
    picked,
    weights,
    outs,
    ins,
    row_buf,
    sum_buf,
    send_sem,
    recv_sem,
    local_sem,
    ring_send,
    ring_recv,
    row_sem,
    sum_sem,
    ready,
    go,
):
    me = lax.axis_index(elem)
    x, y, c = me // (NY * NC), (me // NC) % NY, me % NC
    odd = (x + y + c) % 2
    units = NX * NY * NC
    band_count = bands.shape[0]
    beam_count = table.shape[1]
    dirs, elements = delays.shape
    depth = elements // NX
    own = snap.shape[1] * snap.shape[5]

    def at(px, py, pc):
        return {elem: (px * NY + py) * NC + pc}

    def wrap(v):
        return (v + 2 * NX) % NX

    lead = c == NC - 1
    barrier = pltpu.get_barrier_semaphore()

    def tell(semaphore, target):
        pl.semaphore_signal(semaphore, inc=1, device_id=target, device_id_type=pl.DeviceIdType.MESH)

    def each_lead(act):
        @pl.when(lead)
        def _():
            def one(t, carry):
                act(wrap(x + t), wrap(y + t))
                return carry

            lax.fori_loop(1, NX, one, 0)

    def greet(px, py):
        tell(barrier, at(px, y, c))
        tell(barrier, at(x, py, c))

    tell(barrier, at(x, y, NC - 1 - c))
    each_lead(greet)

    loads = [
        pltpu.make_async_copy(bands, bands_s, local_sem.at[0]),
        pltpu.make_async_copy(order, order_v, local_sem.at[1]),
        pltpu.make_async_copy(table, table_v, local_sem.at[2]),
        pltpu.make_async_copy(delays, delays_v, local_sem.at[3]),
    ]
    for load in loads:
        load.start()
    pl.semaphore_wait(barrier, jnp.where(lead, 2 * (NX - 1) + 1, 1))

    def pass_ready(px, py):
        tell(ready.at[0, x], at(px, y, c))
        tell(ready.at[1, y], at(x, py, c))

    each_lead(pass_ready)

    @pl.when(lead)
    def _():
        tell(go, at(x, y, NC - 1 - c))

    @pl.when(jnp.logical_not(lead))
    def _():
        pl.semaphore_wait(go, 1)

    def send(step, path, px, py, pc):
        role, off = STEPS[step]
        src = (px, wrap(py + off), pc) if path == 0 else (wrap(px + off), py, pc)
        slot = (x if path == 0 else y) * NC + c
        return pltpu.make_async_remote_copy(
            src_ref=snap.at[:, :, src[0], src[1], src[2]],
            dst_ref=recv.at[step, slot],
            send_sem=send_sem,
            recv_sem=recv_sem.at[step],
            device_id=at(px, py, pc),
            device_id_type=pl.DeviceIdType.MESH,
        )

    def keep(step, path):
        role, off = STEPS[step]
        src = (x, wrap(y + off), c) if path == 0 else (wrap(x + off), y, c)
        slot = (x if path == 0 else y) * NC + c
        return pltpu.make_async_copy(
            snap.at[:, :, src[0], src[1], src[2]], recv.at[step, slot], recv_sem.at[step]
        )

    def exchange(step, pc):
        role, off = STEPS[step]
        for path in (0, 1):
            shift = (x + y + pc + (role == "B") + path) % 2
            mine = jnp.logical_and(shift == 0, c == pc)

            def away(j):
                by = shift + 2 * j
                return (wrap(x + by), y) if path == 0 else (x, wrap(y + by))

            @pl.when(mine)
            def _():
                keep(step, path).start()

            @pl.when(jnp.logical_not(mine))
            def _():
                send(step, path, *away(0), pc).start()

            def others(j, carry):
                send(step, path, *away(j), pc).start()
                return carry

            lax.fori_loop(1, NX // 2, others, 0)

    for step in range(AHEAD):
        exchange(step, NC - 1)

    def others_ready(t, carry):
        for axis, chip in ((0, wrap(x + t)), (1, wrap(y + t))):
            pl.semaphore_wait(ready.at[axis, chip], 1)

            @pl.when(lead)
            def _():
                tell(ready.at[axis, chip], at(x, y, NC - 1 - c))

        return carry

    lax.fori_loop(1, NX, others_ready, 0)
    for step in range(AHEAD):
        exchange(step, 0)
    loads[0].wait()
    ends, total = [], jnp.int32(0)
    for b in range(band_count):
        total = total + bands_s[b]
        ends.append(total)

    def unit_of(role, off):
        first = (x * NY + wrap(y + off)) * NC + c
        second = (wrap(x + off) * NY + y) * NC + c
        even = jnp.where(odd == 0, first, second)
        return even if role == "A" else first + second - even

    for step, (role, off) in enumerate(STEPS):
        unit = unit_of(role, off)
        frequency = jnp.float32(0)
        for b in range(band_count):
            start = ends[b] - bands_s[b]
            inside = jnp.logical_and(start <= unit, unit < ends[b])
            middle = start.astype(jnp.float32) + 0.5 * bands_s[b].astype(jnp.float32)
            frequency = frequency + jnp.where(inside, middle, 0.0)
        freq_s[step] = frequency / float(units)

    loads[1].wait()
    loads[2].wait()
    lane = lax.broadcasted_iota(jnp.int32, (8, depth), 1)
    row_order = jnp.zeros((8, depth), jnp.int32)
    group = NC * own
    for px in range(NX):
        part = jnp.broadcast_to(order_v[0:1, px * depth : (px + 1) * depth], (8, depth))
        part = pltpu.roll(part, (px - y + NX) % NX * group, 1)
        row_order = jnp.where(lane // group == px, part, row_order)
    column_order = jnp.broadcast_to(order_v[0:1, pl.ds(pl.multiple_of(x * depth, depth), depth)], (8, depth))
    order_a = jnp.where(odd == 0, row_order, column_order)
    order_b = row_order + column_order - order_a
    both = jnp.concatenate([order_a, order_b], axis=1)[0:1]

    loads[3].wait()
    gathered[...] = jnp.zeros_like(gathered)
    chunk = 256

    def pick_columns(i, carry):
        base = pl.multiple_of(i * chunk, chunk)
        rows = lax.broadcasted_iota(jnp.int32, (chunk, 2 * depth), 0) + base
        hot = jnp.where(rows == both, 1.0, 0.0).astype(jnp.bfloat16)
        one, two, three = split3(delays_v[:, pl.ds(base, chunk)])
        gathered[...] += dot(one, hot) + dot(two, hot) + dot(three, hot)
        return carry

    lax.fori_loop(0, elements // chunk, pick_columns, 0)
    wide = jnp.broadcast_to(table_v[...], (LANES, beam_count)).astype(jnp.float32)
    wide = jnp.transpose(wide)
    hots = []
    for d in range(0, dirs, LANES):
        column = (lax.broadcasted_iota(jnp.int32, (beam_count, LANES), 1) + d).astype(jnp.float32)
        hots.append(jnp.where(wide == column, 1.0, 0.0).astype(jnp.bfloat16))
    hot = jnp.concatenate(hots, axis=1)
    one, two, three = split3(gathered[...])
    rows = dot(hot, one) + dot(hot, two) + dot(hot, three)
    picked[0] = rows[:, :depth]
    picked[1] = rows[:, depth:]

    scale = float(elements) ** -0.5
    block = 32

    def steer(step, role):
        def body(i, carry):
            at_rows = pl.ds(pl.multiple_of(i * block, block), block)
            turns = freq_s[step] * picked[role, at_rows, :]
            nearest = (turns + 12582912.0) - 12582912.0
            r = turns - nearest
            s = r * r
            cosine = horner(COS, s, scale)
            sine = r * horner(SIN, s, scale)
            for n, value in ((0, cosine), (2, sine)):
                high = value.astype(jnp.bfloat16)
                weights[step, n, at_rows, :] = high
                weights[step, n + 1, at_rows, :] = (value - high.astype(jnp.float32)).astype(jnp.bfloat16)
            return carry

        lax.fori_loop(0, beam_count // block, body, 0)

    for step, (role, off) in enumerate(STEPS):
        steer(step, 0 if role == "A" else 1)

    def partial(step):
        pltpu.make_async_copy(recv.at[step], recv.at[step], recv_sem.at[step]).wait()
        data = jnp.concatenate(
            [recv[step, :, 0].reshape(depth, LANES), recv[step, :, 1].reshape(depth, LANES)], axis=1
        )
        high = data.astype(jnp.bfloat16)
        low = (data - high.astype(jnp.float32)).astype(jnp.bfloat16)
        w = weights.at[step]
        cos_part = dot(w[0], high) + dot(w[1], high) + dot(w[0], low)
        sin_part = dot(w[2], high) + dot(w[3], high) + dot(w[2], low)
        real = cos_part[:, :LANES] + sin_part[:, LANES:]
        imag = cos_part[:, LANES:] - sin_part[:, :LANES]
        return real, imag

    def neighbour(role, by):
        px_a = jnp.where(odd == 0, x, wrap(x + by))
        py_a = jnp.where(odd == 0, wrap(y + by), y)
        px_b = jnp.where(odd == 0, wrap(x + by), x)
        py_b = jnp.where(odd == 0, y, wrap(y + by))
        return at(px_a, py_a, c) if role == "A" else at(px_b, py_b, c)

    def pass_on(step, q, buf):
        role, off = STEPS[step]
        by = 1 if buf in (P3, P2, P1, P0) else -1
        return pltpu.make_async_remote_copy(
            src_ref=outs.at[step, q],
            dst_ref=ins.at[buf, q],
            send_sem=ring_send,
            recv_sem=ring_recv.at[buf, q],
            device_id=neighbour(role, by),
            device_id_type=pl.DeviceIdType.MESH,
        )

    def arrived(buf, q):
        pltpu.make_async_copy(ins.at[buf, q], ins.at[buf, q], ring_recv.at[buf, q]).wait()
        return ins[buf, q]

    piece = 2 * beam_count // QUARTERS

    def compute(step):
        real, imag = partial(step)
        for h, value in enumerate((real, imag)):
            for q in range(QUARTERS // 2):
                outs[step, h * (QUARTERS // 2) + q] = value[q * piece : (q + 1) * piece]

    low, high = range(QUARTERS // 2), range(QUARTERS // 2, QUARTERS)
    compute(0)
    for q in low:
        pass_on(0, q, P3).start()
    for q in high:
        pass_on(0, q, M3).start()
    compute(1)
    for q in high:
        pass_on(1, q, P2).start()
    compute(2)
    for q in low:
        pass_on(2, q, M2).start()
    compute(3)
    for p, m in zip(low, high):
        outs[1, p] += arrived(P3, p)
        pass_on(1, p, P2).start()
        outs[2, m] += arrived(M3, m)
        pass_on(2, m, M2).start()
    compute(4)
    up, down = (*high, *low), (*low, *high)
    for p, m in zip(up, down):
        outs[3, p] += arrived(P2, p)
        pass_on(3, p, P1).start()
        outs[4, m] += arrived(M2, m)
        pass_on(4, m, M1).start()
    for pc in range(NC):
        exchange(7, pc)
    compute(5)
    compute(6)
    for p, m in zip(up, down):
        outs[5, p] += arrived(P1, p)
        pass_on(5, p, P0).start()
        outs[6, m] += arrived(M1, m)
        pass_on(6, m, M0).start()
    compute(7)
    parts = [jnp.zeros((piece, LANES), jnp.float32) for _ in low]
    for q in up:
        value = outs[7, q] + arrived(P0, q) + arrived(M0, q)
        k = q % len(low)
        beams_out[q // len(low), k * piece : (k + 1) * piece] = value
        parts[k] = parts[k] + value * value
    squares = jnp.concatenate(parts, axis=0)

    unit = unit_of("A", 0)
    size = jnp.float32(0)
    for b in range(band_count):
        inside = jnp.logical_and(ends[b] - bands_s[b] <= unit, unit < ends[b])
        size = size + jnp.where(inside, bands_s[b].astype(jnp.float32), 0.0)
    ones = jnp.full((8, LANES), 1.0, jnp.bfloat16)
    sums = jnp.zeros((8, beam_count), jnp.float32)
    for piece in split3(squares):
        sums = sums + lax.dot_general(ones, piece, (((1,), (1,)), ((), ())), preferred_element_type=jnp.float32)
    mine = sums / jnp.full((8, beam_count), size * float(LANES), jnp.float32)
    slot = y * NC + c
    row_buf[slot] = mine[0:1]

    def far_first(t, length):
        return length // 2 + jnp.where(t % 2 == 0, t // 2, -(t // 2))

    def row_copy(t):
        s = (slot + far_first(t, RING)) % RING
        return pltpu.make_async_remote_copy(
            src_ref=row_buf.at[slot],
            dst_ref=row_buf.at[slot],
            send_sem=send_sem,
            recv_sem=row_sem,
            device_id=at(x, s // NC, s % NC),
            device_id_type=pl.DeviceIdType.MESH,
        )

    def start_rows(t, carry):
        row_copy(t).start()
        return carry

    lax.fori_loop(1, RING, start_rows, 0)

    band = lax.broadcasted_iota(jnp.int32, (8, beam_count), 0)
    first, last = jnp.zeros_like(band), jnp.zeros_like(band)
    for b in range(band_count):
        first = jnp.where(band == b, ends[b] - bands_s[b], first)
        last = jnp.where(band == b, ends[b], last)
    pltpu.make_async_copy(
        row_buf.at[pl.ds(0, RING - 1)], row_buf.at[pl.ds(0, RING - 1)], row_sem
    ).wait()
    mean = jnp.zeros((8, beam_count), jnp.float32)
    for s in range(RING):
        u = x * RING + s
        inside = jnp.logical_and(first <= u, u < last)
        mean = mean + jnp.where(inside, jnp.broadcast_to(row_buf[s], (8, beam_count)), 0.0)
    sum_buf[x] = mean

    def sum_copy(t):
        return pltpu.make_async_remote_copy(
            src_ref=sum_buf.at[x],
            dst_ref=sum_buf.at[x],
            send_sem=send_sem,
            recv_sem=sum_sem,
            device_id=at(wrap(x + far_first(t, NX)), y, c),
            device_id_type=pl.DeviceIdType.MESH,
        )

    def start_sums(t, carry):
        sum_copy(t).start()
        return carry

    lax.fori_loop(1, NX, start_sums, 0)
    pltpu.make_async_copy(
        sum_buf.at[pl.ds(0, NX - 1)], sum_buf.at[pl.ds(0, NX - 1)], sum_sem
    ).wait()
    total = sum_buf[0]
    for s in range(1, NX):
        total = total + sum_buf[s]
    power_out[...] = 10.0 * (jnp.log(total + epsilon) * (1.0 / math.log(10.0)))

    for step in range(7):
        pltpu.make_async_copy(recv.at[step], recv.at[step], send_sem).wait()
    half_ring = recv.at[7, pl.ds(0, RING // 2)]
    pltpu.make_async_copy(half_ring, half_ring, send_sem).wait()
    rows = row_buf.at[pl.ds(0, RING - 1)]
    pltpu.make_async_copy(rows, rows, send_sem).wait()
    rows = sum_buf.at[pl.ds(0, NX - 1)]
    pltpu.make_async_copy(rows, rows, send_sem).wait()
    rows = outs.at[pl.ds(0, 7)]
    pltpu.make_async_copy(rows, rows, ring_send).wait()


def local(elem, snapshots, delays, element_order, beam_table, band_len):
    planes, own, columns = snapshots.shape
    tiles = columns // LANES
    view = snapshots.reshape(planes, own // 8, 8, tiles, LANES).transpose(0, 1, 3, 2, 4)
    view = view.reshape(planes, own // 8, NX, NY, NC, 8, LANES)
    beam_count, elements = beam_table.shape[0], delays.shape[1]
    depth = elements // NX
    unit = (RING, planes, own // 8, 8, LANES)
    operands = (view, delays, element_order.reshape(1, elements), beam_table.reshape(1, beam_count), band_len)
    formed, decibels = pl.pallas_call(
        functools.partial(kernel, elem),
        out_shape=(
            jax.ShapeDtypeStruct((2, beam_count, LANES), jnp.float32),
            jax.ShapeDtypeStruct((band_len.shape[0], beam_count), jnp.float32),
        ),
        in_specs=[pl.BlockSpec(memory_space=pltpu.HBM)] * 5,
        out_specs=(pl.BlockSpec(memory_space=pltpu.VMEM), pl.BlockSpec(memory_space=pltpu.VMEM)),
        scratch_shapes=[
            pltpu.VMEM((8, *unit), jnp.float32),
            pltpu.VMEM(delays.shape, jnp.float32),
            pltpu.VMEM((1, elements), jnp.int32),
            pltpu.VMEM((1, beam_count), jnp.int32),
            pltpu.SMEM(band_len.shape, jnp.int32),
            pltpu.SMEM((8,), jnp.float32),
            pltpu.VMEM((delays.shape[0], 2 * depth), jnp.float32),
            pltpu.VMEM((2, beam_count, depth), jnp.float32),
            pltpu.VMEM((8, 4, beam_count, depth), jnp.bfloat16),
            pltpu.VMEM((8, QUARTERS, 2 * beam_count // QUARTERS, LANES), jnp.float32),
            pltpu.VMEM((8, QUARTERS, 2 * beam_count // QUARTERS, LANES), jnp.float32),
            pltpu.VMEM((RING, 1, beam_count), jnp.float32),
            pltpu.VMEM((NX, band_len.shape[0], beam_count), jnp.float32),
            pltpu.SemaphoreType.DMA(()),
            pltpu.SemaphoreType.DMA((8,)),
            pltpu.SemaphoreType.DMA((4,)),
            pltpu.SemaphoreType.DMA(()),
            pltpu.SemaphoreType.DMA((8, QUARTERS)),
            pltpu.SemaphoreType.DMA(()),
            pltpu.SemaphoreType.DMA(()),
            pltpu.SemaphoreType.REGULAR((2, NX)),
            pltpu.SemaphoreType.REGULAR,
        ],
        compiler_params=pltpu.CompilerParams(
            collective_id=1, has_side_effects=True, vmem_limit_bytes=48 * 1024 * 1024
        ),
    )(*(pltpu.with_memory_space_constraint(a, pltpu.HBM) for a in operands))
    return formed.transpose(2, 0, 1), decibels


def solution(mesh):
    return jax.shard_map(
        functools.partial(local, "elem"),
        mesh=mesh,
        in_specs=(P(None, ("groups", "elem"), None), P(), P("groups"), P("groups"), P()),
        out_specs=(P("elem", None, "groups"), P(None, "groups")),
        check_vma=False,
    )
```
